128 devices in a mesh: grp: 4 (over y), row: 32 (over z, x, core).
Axes of the slice: x: 4, y: 4, z: 4, core: 2. Of those that a mesh axis runs over, the one named last changes fastest.
Arguments:
- tiles: bfloat16 [4, 32, 32, 256, 256], P('grp', 'row'), may hold values from -0.046875 to 0.046875
- tile_rows: int32 [4, 32, 32], P('grp', 'row'), may hold values from 0 to 3, as said below
- tile_cols: int32 [4, 32, 32], P('grp', 'row'), may hold values from 0 to 31, as said below
- live_tiles: int32 [4, 32], P('grp', 'row'), may hold values from 16 to 32, as said below
- dual_shift: float32 [32768], P('row'), may hold values from 0.5 to 2
- start_block: float32 [32, 32768], P(None, 'row'), may hold values from -6 to 6
Outputs:
- projections: float32 [4, 32, 128], replicated
- factors: float32 [4, 32, 32], replicated
- next_block: float32 [32, 32768], P(None, 'row')
The draws below stay inside these ranges and needn't reach their ends.
Inputs may be any that keep to these rules, and one draw needn't show every extreme that they name: `tile_rows`: the tile slots of one device sit at distinct positions (block row, column block), padding slots included. `tile_cols`: column block j of group g is global block column (j // 1) * 4 + g * 1 + j % 1. Slots from live_tiles on are padding with arbitrary values; in every draw some device has all 32 slots live.
All inputs are finite; a program needn't handle non-finite values.
Results may differ from the reference program's by a relative error of at most 0.013.
Values may be sent and summed in bfloat16 or wider, within the bound.
A program may use at most 64 MiB of HBM per device.

```python
import math
import jax
import jax.numpy as jnp
from jax import lax

K = 32
BS = 256
BR_DEV = 4
KB = 32
ITERS = 4
N = 32768
QB = 1
NCG = 32
M = 128
N_GRP = 4
N_ROW = 32


def tile_slots(key):
    keys = jax.random.split(jax.random.fold_in(key, 7), N_GRP * N_ROW)
    slots = jax.vmap(lambda one_key: jax.random.permutation(one_key, BR_DEV * NCG)[:KB])(keys)
    return slots.reshape(N_GRP, N_ROW, KB).astype(jnp.int32)


def draw_tile_rows(key, part):
    return (tile_slots(key) // NCG).astype(jnp.int32)


def draw_tile_cols(key, part):
    return (tile_slots(key) % NCG).astype(jnp.int32)


def draw_live_tiles(key, part):
    count_key = jax.random.fold_in(key, 11)
    pick_key = jax.random.fold_in(key, 13)
    counts = jax.random.randint(count_key, (N_GRP * N_ROW,), KB // 2, KB + 1)
    picked = jax.random.randint(pick_key, (), 0, N_GRP * N_ROW)
    counts = jnp.where(jnp.arange(N_GRP * N_ROW) == picked, KB, counts)
    return counts.reshape(N_GRP, N_ROW).astype(jnp.int32)


def steps_of(own_key, shape, pieces, low, largest):
    level = 1.0
    for dim, shards_of in pieces:
        heights = jax.random.uniform(jax.random.fold_in(jax.random.fold_in(own_key, 6), dim), (shards_of,), jnp.float32, low / len(pieces), largest / len(pieces))
        level = level * jnp.repeat(jnp.exp(heights), shape[dim] // shards_of).reshape((-1,) + (1,) * (len(shape) - 1 - dim))
    return level


def noise(key, shape, width, reach, shards=(), dtype=jnp.bfloat16):
    array = jax.random.normal(key, shape, jnp.float32) * width
    if len(shards) > 0:
        array = steps_of(key, shape, shards, -0.22, 0.18) * array
    return jnp.clip(array, min=-reach, max=reach).astype(dtype)


def setup_inputs(seed: int = 0) -> dict:
    seeds = jax.random.split(jax.random.key(seed), 7)
    return {
        "tiles": noise(seeds[0], (N_GRP, N_ROW, KB, BS, BS), (KB * N_GRP * 2 * BS // BR_DEV) ** -0.5, 0.046875, ((0, 4), (1, 32))),
        "tile_rows": draw_tile_rows(jax.random.fold_in(seeds[6], 71), 0),
        "tile_cols": draw_tile_cols(jax.random.fold_in(seeds[6], 71), 0),
        "live_tiles": draw_live_tiles(jax.random.fold_in(seeds[6], 71), 0),
        "dual_shift": jnp.clip(jnp.exp(math.log(2.0) - 1.3862944 * jax.random.uniform(seeds[4], (N,), jnp.float32) ** steps_of(seeds[4], (N,), ((0, 32),), -0.2, 0.2)), 0.5, 2.0),
        "start_block": noise(seeds[5], (K, N), 1.0, 6.0, ((1, 32),), jnp.float32),
    }


def inner_product(left, right):
    return lax.dot_general(left.astype(jnp.float32), right.astype(jnp.float32), (((1,), (1,)), ((), ())), precision=lax.Precision.HIGHEST, preferred_element_type=jnp.float32)

def apply_matrix(left, right):
    return jnp.dot(left.astype(jnp.float32), right.astype(jnp.float32), precision=lax.Precision.HIGHEST, preferred_element_type=jnp.float32)

def operate(vectors, tiles, tile_rows, tile_cols, live_tiles):
    rounded = vectors.astype(jnp.bfloat16).astype(jnp.float32).reshape(K, N_ROW, BR_DEV, BS)

    def visit(device, totals):
        direct_sum, back_sum = totals
        group = (device // N_ROW).astype(jnp.int32)
        owner = (device % N_ROW).astype(jnp.int32)
        matrix = tiles[group, owner].astype(jnp.float32)
        rows_here = tile_rows[group, owner]
        cols_here = tile_cols[group, owner]
        live_mask = (jnp.arange(KB) < live_tiles[group, owner]).astype(jnp.float32)
        column_part = lax.dynamic_slice_in_dim(rounded, group * QB, QB, 2).reshape(K, NCG, BS)
        own_part = lax.dynamic_index_in_dim(rounded, owner, 1, False)
        forward = jnp.einsum('kbc,brc->kbr', column_part[:, cols_here], matrix)
        row_table = (rows_here[:, None] == jnp.arange(BR_DEV)[None, :]).astype(jnp.float32) * live_mask[:, None]
        direct = jnp.einsum('kbr,bi->kir', forward, row_table)
        backward = jnp.einsum('kbr,brc->kbc', own_part[:, rows_here], matrix)
        col_table = (cols_here[:, None] == jnp.arange(NCG)[None, :]).astype(jnp.float32) * live_mask[:, None]
        spread = jnp.einsum('kbc,bj->kjc', backward, col_table).reshape(K, N_ROW, QB, BS)
        old_direct = lax.dynamic_index_in_dim(direct_sum, owner, 1, False)
        direct_sum = lax.dynamic_update_index_in_dim(direct_sum, old_direct + direct, owner, 1)
        old_back = lax.dynamic_index_in_dim(back_sum, group, 2, False)
        back_sum = lax.dynamic_update_index_in_dim(back_sum, old_back + spread, group, 2)
        return (direct_sum, back_sum)
    begin = (jnp.zeros((K, N_ROW, BR_DEV, BS), jnp.float32), jnp.zeros((K, N_ROW, N_GRP, QB, BS), jnp.float32))
    direct_sum, back_sum = lax.fori_loop(0, N_GRP * N_ROW, visit, begin)
    return 0.5 * (direct_sum.reshape(K, N) + back_sum.reshape(K, N))

def orthonormal(block):
    lower_factor = jnp.linalg.cholesky(inner_product(block, block))
    return (lax.linalg.triangular_solve(lower_factor, block, left_side=True, lower=True), lower_factor)

def reference(tiles, tile_rows, tile_cols, live_tiles, dual_shift, start_block):
    current, unused = orthonormal(start_block)
    basis_rows = jnp.zeros((M, N), jnp.float32)
    proj_list = []
    factor_list = []
    for step_index in range(ITERS):
        basis_rows = basis_rows.at[step_index * K:(step_index + 1) * K].set(current)
        image = operate(current, tiles, tile_rows, tile_cols, live_tiles) - current * dual_shift[None, :]
        first_coef = inner_product(image, basis_rows)
        image = image - apply_matrix(first_coef, basis_rows)
        current, lower_factor = orthonormal(image)
        proj_list.append(first_coef)
        factor_list.append(lower_factor)
    return (jnp.stack(proj_list), jnp.stack(factor_list), current)
```

```python
import functools

import jax
import jax.numpy as jnp
from jax import lax
from jax.experimental import pallas as pl
from jax.experimental.pallas import tpu as pltpu
from jax.sharding import PartitionSpec as P

MESH = pl.DeviceIdType.MESH
HIGHEST = lax.Precision.HIGHEST
F32 = jnp.float32
BF16 = jnp.bfloat16

ITERS = 4
K = 32
BS = 256
GRP = 4
ROW = 32
CHIPS = ROW // 2
SIDE = 4
TILES = 32
SHIFT = -1.0

FAR_FIRST = sorted(
    [(dz, dx) for dz in range(SIDE) for dx in range(SIDE) if (dz, dx) != (0, 0)],
    key=lambda d: -(min(d[0], SIDE - d[0]) + min(d[1], SIDE - d[1])),
)
SMALL_GROUP = [(dy, dc) for dy in (2, 1, 3, 0) for dc in (1, 0) if (dy, dc) != (0, 0)]


def height(step):
    return 2 * K if step == 0 else K


def dot(left, right, precision=None):
    return lax.dot_general(
        left, right, (((1,), (0,)), ((), ())), precision=precision, preferred_element_type=F32
    )


def dot_t(left, right, precision=None):
    return lax.dot_general(
        left, right, (((1,), (1,)), ((), ())), precision=precision, preferred_element_type=F32
    )


def cholesky(gram):
    row = lax.broadcasted_iota(jnp.int32, (K, K), 0)
    col = lax.broadcasted_iota(jnp.int32, (K, K), 1)
    left = gram
    right = jnp.where(row == col, 1.0, 0.0).astype(F32)
    for k in range(K - 1):
        factor = jnp.broadcast_to(left[:, k : k + 1], (K, K)) / left[k : k + 1, k : k + 1]
        factor = jnp.where(row > k, factor, 0.0)
        left = left - factor * left[k : k + 1, :]
        right = right - factor * right[k : k + 1, :]
    pivots = jnp.sum(jnp.where(row == col, left, 0.0), axis=1, keepdims=True)
    scale = 1.0 / jnp.sqrt(pivots)
    return jnp.where(col >= row, left * scale, 0.0), right * scale


def kernel(
    slot_ref,
    rows_ref,
    cols_ref,
    tiles_hbm,
    start_ref,
    dual_ref,
    proj_ref,
    fact_ref,
    next_ref,
    tiles,
    cols_0,
    cols_1,
    cols_2,
    cols_3,
    cols_4,
    rows_0,
    rows_1,
    rows_2,
    rows_3,
    raw_x,
    raw_y,
    trans,
    products,
    pair_out,
    pair_in,
    back_out,
    back_in,
    own_back,
    direct_out,
    direct_in,
    dots,
    tile_sem,
    cols_send,
    cols_recv,
    relay_send,
    relay_recv,
    rows_send,
    rows_recv,
    raw_send,
    raw_recv,
    dots_send,
    dots_recv,
    pair_send,
    pair_recv,
    back_send,
    back_recv,
    direct_send,
    direct_recv,
):
    cols_x = (cols_0, cols_1, cols_2, cols_3, cols_4)
    rows_x = (rows_0, rows_1, rows_2, rows_3)
    g = lax.axis_index("grp")
    r = lax.axis_index("row")
    core = lax.rem(r, 2)
    chip = lax.div(r, 2)
    z = lax.div(chip, SIDE)
    x = lax.rem(chip, SIDE)
    partner = r + 1 - 2 * core

    def chip_at(dz, dx):
        return lax.rem(z + dz, SIDE) * SIDE + lax.rem(x + dx, SIDE)

    def chip_from(dz, dx):
        return lax.rem(z + SIDE - dz, SIDE) * SIDE + lax.rem(x + SIDE - dx, SIDE)

    def remote(src, dst, send, recv, group, owner):
        return pltpu.make_async_remote_copy(
            src_ref=src,
            dst_ref=dst,
            send_sem=send,
            recv_sem=recv,
            device_id=(group, owner),
            device_id_type=MESH,
        )

    def await_recv(ref, send, recv):
        remote(ref, ref, send, recv, g, partner).wait_recv()

    def await_send(ref, send, recv):
        remote(ref, ref, send, recv, g, partner).wait_send()

    load = pltpu.make_async_copy(tiles_hbm, tiles, tile_sem)
    load.start()

    barrier = pltpu.get_barrier_semaphore()
    for dz, dx in FAR_FIRST:
        pl.semaphore_signal(
            barrier, inc=1, device_id=(g, chip_at(dz, dx) * 2 + core), device_id_type=MESH
        )
    for dy, dc in SMALL_GROUP:
        pl.semaphore_signal(
            barrier,
            inc=1,
            device_id=(lax.rem(g + dy, GRP), partner if dc else r),
            device_id_type=MESH,
        )

    for i in range(GRP):
        block = start_ref[:, i * BS : (i + 1) * BS]
        high = block.astype(BF16)
        rows_0[i, 0:K, :] = high
        rows_0[i, K : 2 * K, :] = (block - high.astype(F32)).astype(BF16)
        raw_x[i, 0:K, :] = block
    cols_0[r] = rows_0[g]
    trans[...] = jnp.zeros_like(trans)
    products[TILES] = jnp.zeros((K, BS), F32)
    proj_ref[...] = jnp.zeros_like(proj_ref)
    dual = dual_ref[:, pl.ds(pl.multiple_of(g * BS, BS), BS)]

    def send_cols(step):
        here = cols_x[step].at[r]
        for m, (dz, dx) in enumerate(FAR_FIRST):
            remote(
                here, here, cols_send.at[step], cols_recv.at[step, m], g, chip_at(dz, dx) * 2 + core
            ).start()
        if step < ITERS:
            remote(here, here, relay_send.at[step], relay_recv.at[step], g, partner).start()

    def receive_cols(step):
        for m in reversed(range(len(FAR_FIRST))):
            source = chip_from(*FAR_FIRST[m]) * 2 + core
            there = cols_x[step].at[source]
            await_recv(there, cols_send.at[step], cols_recv.at[step, m])
            if step < ITERS:
                remote(there, there, relay_send.at[step], relay_recv.at[step], g, partner).start()

    def products_of(load_left, rows, transposed):
        def body(k, carry):
            tile = tiles[k]
            product = dot_t(load_left(k), tile) if transposed else dot(load_left(k), tile)
            if rows == 2 * K:
                product = product[:K] + product[K:]
            products[k] = product
            return carry

        lax.fori_loop(0, TILES, body, 0, unroll=8)

    def back_sum(owner):
        total = products[slot_ref[owner]]
        for i in range(1, GRP):
            total = total + products[slot_ref[i * ROW + owner]]
        return total

    def send_pairs(step):
        def other(m, carry):
            pair_out[step, m] = back_sum(m * 2 + 1 - core).astype(BF16)
            return carry

        lax.fori_loop(0, CHIPS, other, 0, unroll=2)
        remote(
            pair_out.at[step],
            pair_in.at[step],
            pair_send.at[step],
            pair_recv.at[step],
            g,
            partner,
        ).start()

    def send_back(step):
        def mine(m, carry):
            own_back[m] = back_sum(m * 2 + core)
            return carry

        lax.fori_loop(0, CHIPS, mine, 0, unroll=2)
        await_recv(pair_in.at[step], pair_send.at[step], pair_recv.at[step])
        for dz, dx in FAR_FIRST:
            there = chip_at(dz, dx)
            back_out[step, there] = (
                own_back[there] + pair_in[step, there].astype(F32)
            ).astype(BF16)
        for dz, dx in FAR_FIRST:
            there = chip_at(dz, dx)
            remote(
                back_out.at[step, there],
                back_in.at[step, chip],
                back_send.at[step],
                back_recv.at[step],
                g,
                there * 2 + core,
            ).start()

    def send_direct(step):
        for i in range(GRP):

            def add(j, total, i=i):
                return total + products[slot_ref[i * ROW + j]]

            direct_out[step, i] = lax.fori_loop(
                0, ROW, add, jnp.zeros((K, BS), F32), unroll=8
            )
        for dy in (2, 1, 3):
            group = lax.rem(g + dy, GRP)
            remote(
                direct_out.at[step, group],
                direct_in.at[step, g],
                direct_send.at[step],
                direct_recv.at[step],
                group,
                r,
            ).start()

    def send_dots(step):
        size = height(step)
        width = K * step + 2 * K if step else 2 * K

        def add(p, total):
            owner = p * 2 + core
            so_far = jnp.concatenate([cols_x[s][owner] for s in range(step + 1)], axis=0)
            return total + dot_t(cols_x[step][owner], so_far)

        total = lax.fori_loop(0, CHIPS, add, jnp.zeros((size, width), F32), unroll=4)
        here = g * 2 + core
        if step == 0:
            dots[0, here, :, 0:K] = (total[:K, :K] + total[:K, K:]) + (
                total[K:, :K] + total[K:, K:]
            )
        else:
            dots[step, here, :, 0:K] = total[:, 0:K] + total[:, K : 2 * K]
            dots[step, here, :, K : K + K * step] = total[:, 2 * K :]
        lanes = 128 if step < ITERS else 256
        mine = dots.at[step, here, :, pl.ds(0, lanes)]
        for dy, dc in SMALL_GROUP:
            remote(
                mine,
                mine,
                dots_send.at[step],
                dots_recv.at[step],
                lax.rem(g + dy, GRP),
                partner if dc else r,
            ).start()

    def receive_dots(step):
        lanes = 128 if step < ITERS else 256
        await_recv(
            dots.at[step, pl.ds(0, 7), :, pl.ds(0, lanes)], dots_send.at[step], dots_recv.at[step]
        )
        total = dots[step, 0, :, 0 : K + K * step]
        for i in range(1, 2 * GRP):
            total = total + dots[step, i, :, 0 : K + K * step]
        gram = total[:, K * step :]
        if step > 0:
            before = trans[0 : K * step, 0 : K * step]
            coef = dot_t(total[:, : K * step], before, HIGHEST)
            gram = gram - dot_t(coef, coef, HIGHEST)
        upper, inverse = cholesky(gram)
        trans[K * step : K * step + K, K * step : K * step + K] = inverse
        if step > 0:
            trans[K * step : K * step + K, 0 : K * step] = -dot(
                inverse, dot(coef, before, HIGHEST), HIGHEST
            )
            fact_ref[step - 1] = upper.T
        return coef if step > 0 else None, upper, inverse

    def record(step, coef, upper_before):
        row = lax.broadcasted_iota(jnp.int32, (K, K), 0)
        col = lax.broadcasted_iota(jnp.int32, (K, K), 1)
        at = K * (step - 1)
        if step > 1:
            proj_ref[step - 1, :, 0:at] = coef[:, :at]
            proj_ref[step - 1, :, at - K : at] = coef[:, at - K : at] + upper_before
        proj_ref[step - 1, :, at : at + K] = coef[:, at:] + jnp.where(row == col, SHIFT, 0.0)

    upper_before = None
    for step in range(ITERS):
        size = height(step)
        if step == 0:
            load.wait()
            products_of(lambda k: rows_0[rows_ref[k]], size, False)
            pl.semaphore_wait(barrier, len(FAR_FIRST) + len(SMALL_GROUP))
            send_cols(0)
            send_pairs(0)
        else:
            await_recv(rows_x[step].at[pl.ds(0, 3)], rows_send.at[step], rows_recv.at[step])
            products_of(lambda k, step=step: rows_x[step][rows_ref[k]], size, False)
            send_pairs(step)
        send_back(step)

        receive_cols(step)
        send_dots(step)
        await_recv(cols_x[step].at[pl.ds(0, CHIPS)], relay_send.at[step], relay_recv.at[step])
        products_of(lambda k, step=step: cols_x[step][cols_ref[k]], size, True)
        send_direct(step)

        coef, upper, inverse = receive_dots(step)
        if step > 0:
            record(step, coef, upper_before)
        here = trans[K * step : K * step + K, 0 : K + K * step]
        known = dot(here, raw_x[g, 0 : K + K * step, :], HIGHEST) * (-SHIFT)
        if step > 0:
            older = dot(
                trans[K * (step - 1) : K * step, 0 : K * step], raw_x[g, 0 : K * step, :], HIGHEST
            )
            known = known - dot(upper, older, HIGHEST)
            known = known + dot(here[:, : K * step], raw_y[0 : K * step, :], HIGHEST)
        upper_before = upper

        await_recv(
            direct_in.at[step, pl.ds(0, 3)], direct_send.at[step], direct_recv.at[step]
        )
        total = direct_out[step, g]
        for dy in (1, 2, 3):
            total = total + direct_in[step, lax.rem(g + dy, GRP)]
        await_recv(back_in.at[step, pl.ds(0, CHIPS - 1)], back_send.at[step], back_recv.at[step])
        total = total + own_back[chip] + pair_in[step, chip].astype(F32)
        for dz, dx in FAR_FIRST:
            total = total + back_in[step, chip_at(dz, dx)].astype(F32)
        image = 0.5 * total - raw_x[g, K * step : K * step + K, :] * dual
        raw_y[K * step : K * step + K, :] = image
        block = dot(inverse, image, HIGHEST) + known
        rounded = block.astype(BF16)
        after = step + 1
        cols_x[after][r] = rounded
        raw_x[g, K * after : K * after + K, :] = block
        if after < ITERS:
            rows_x[after][g] = rounded
            mine = rows_x[after].at[g]
            for dy in (2, 1, 3):
                remote(
                    mine, mine, rows_send.at[after], rows_recv.at[after], lax.rem(g + dy, GRP), r
                ).start()
        send_cols(after)
        mine = raw_x.at[g, pl.ds(K * after, K), :]
        for dy in (2, 1, 3):
            remote(
                mine, mine, raw_send.at[after], raw_recv.at[after], lax.rem(g + dy, GRP), r
            ).start()

    receive_cols(ITERS)
    send_dots(ITERS)
    coef, upper, inverse = receive_dots(ITERS)
    record(ITERS, coef, upper_before)
    for step in range(1, ITERS + 1):
        await_recv(
            raw_x.at[pl.ds(0, 3), pl.ds(K * step, K), :], raw_send.at[step], raw_recv.at[step]
        )
    final = trans[K * ITERS : K * ITERS + K, :]
    for i in range(GRP):
        next_ref[:, i * BS : (i + 1) * BS] = dot(final, raw_x[i], HIGHEST)

    for step in range(ITERS + 1):
        await_send(cols_x[step].at[pl.ds(0, CHIPS - 1)], cols_send.at[step], cols_recv.at[step, 0])
        lanes = 128 if step < ITERS else 256
        await_send(
            dots.at[step, pl.ds(0, 7), :, pl.ds(0, lanes)], dots_send.at[step], dots_recv.at[step]
        )
        if step > 0:
            await_send(
                raw_x.at[pl.ds(0, 3), pl.ds(K * step, K), :], raw_send.at[step], raw_recv.at[step]
            )
        if step == ITERS:
            continue
        await_send(cols_x[step].at[pl.ds(0, CHIPS)], relay_send.at[step], relay_recv.at[step])
        await_send(pair_out.at[step], pair_send.at[step], pair_recv.at[step])
        await_send(back_in.at[step, pl.ds(0, CHIPS - 1)], back_send.at[step], back_recv.at[step])
        await_send(direct_in.at[step, pl.ds(0, 3)], direct_send.at[step], direct_recv.at[step])
        if step > 0:
            await_send(rows_x[step].at[pl.ds(0, 3)], rows_send.at[step], rows_recv.at[step])


def per_device(tiles, tile_rows, tile_cols, live_tiles, dual_shift, start_block):
    rows = tile_rows[0, 0]
    cols = tile_cols[0, 0]
    number = jnp.arange(TILES, dtype=jnp.int32)
    place = jnp.where(number < live_tiles[0, 0], rows * ROW + cols, -1)
    slot = TILES - jnp.sum(
        jnp.where(
            place[None, :] == jnp.arange(GRP * ROW, dtype=jnp.int32)[:, None],
            TILES - number[None, :],
            0,
        ),
        axis=1,
    )
    smem = pl.BlockSpec(memory_space=pltpu.SMEM)
    vmem = pl.BlockSpec(memory_space=pltpu.VMEM)
    dma = pltpu.SemaphoreType.DMA
    steps = ITERS + 1
    return pl.pallas_call(
        kernel,
        out_shape=(
            jax.ShapeDtypeStruct((ITERS, K, ITERS * K), F32),
            jax.ShapeDtypeStruct((ITERS, K, K), F32),
            jax.ShapeDtypeStruct((K, GRP * BS), F32),
        ),
        in_specs=[smem, smem, smem, pl.BlockSpec(memory_space=pl.ANY), vmem, vmem],
        out_specs=(vmem, vmem, vmem),
        scratch_shapes=[
            pltpu.VMEM((TILES, BS, BS), BF16),
            *[pltpu.VMEM((ROW, height(step), BS), BF16) for step in range(steps)],
            *[pltpu.VMEM((GRP, height(step), BS), BF16) for step in range(ITERS)],
            pltpu.VMEM((GRP, K * steps, BS), F32),
            pltpu.VMEM((K * ITERS, BS), F32),
            pltpu.VMEM((K * steps, K * steps), F32),
            pltpu.VMEM((TILES + 1, K, BS), F32),
            pltpu.VMEM((ITERS, CHIPS, K, BS), BF16),
            pltpu.VMEM((ITERS, CHIPS, K, BS), BF16),
            pltpu.VMEM((ITERS, CHIPS, K, BS), BF16),
            pltpu.VMEM((ITERS, CHIPS, K, BS), BF16),
            pltpu.VMEM((CHIPS, K, BS), F32),
            pltpu.VMEM((ITERS, GRP, K, BS), F32),
            pltpu.VMEM((ITERS, GRP, K, BS), F32),
            pltpu.VMEM((steps, 2 * GRP, K, 256), F32),
            dma,
            dma((steps,)),
            dma((steps, CHIPS - 1)),
            dma((ITERS,)),
            dma((ITERS,)),
            dma((ITERS,)),
            dma((ITERS,)),
            dma((steps,)),
            dma((steps,)),
            dma((steps,)),
            dma((steps,)),
            dma((ITERS,)),
            dma((ITERS,)),
            dma((ITERS,)),
            dma((ITERS,)),
            dma((ITERS,)),
            dma((ITERS,)),
        ],
        compiler_params=pltpu.CompilerParams(
            collective_id=0, has_side_effects=True, vmem_limit_bytes=60 * 1024 * 1024
        ),
        name="lanczos",
    )(
        slot.astype(jnp.int32),
        rows,
        cols,
        tiles.reshape(TILES, BS, BS),
        start_block,
        dual_shift.reshape(1, GRP * BS),
    )


def solution(mesh):
    in_specs = (
        P("grp", "row", None, None, None),
        P("grp", "row", None),
        P("grp", "row", None),
        P("grp", "row"),
        P("row"),
        P(None, "row"),
    )
    out_specs = (P(), P(), P(None, "row"))
    return jax.shard_map(
        per_device, mesh=mesh, in_specs=in_specs, out_specs=out_specs, check_vma=False
    )
```

```python
import functools

import jax
import jax.numpy as jnp
from jax import lax
from jax.experimental import pallas as pl
from jax.experimental.pallas import tpu as pltpu
from jax.sharding import PartitionSpec as P

MESH = pl.DeviceIdType.MESH
HIGHEST = lax.Precision.HIGHEST
F32 = jnp.float32
BF16 = jnp.bfloat16

ITERS = 4
K = 32
BS = 256
GRP = 4
ROW = 32
CHIPS = ROW // 2
SIDE = 4
TILES = 32
SHIFT = -1.0

FAR_FIRST = sorted(
    [(dz, dx) for dz in range(SIDE) for dx in range(SIDE) if (dz, dx) != (0, 0)],
    key=lambda d: -(min(d[0], SIDE - d[0]) + min(d[1], SIDE - d[1])),
)
SMALL_GROUP = [(dy, dc) for dy in (2, 1, 3, 0) for dc in (1, 0) if (dy, dc) != (0, 0)]


def height(step):
    return 2 * K if step == 0 else K


def dots_height(step):
    return K if step < ITERS else K + 8


def dot(left, right, precision=None):
    return lax.dot_general(
        left, right, (((1,), (0,)), ((), ())), precision=precision, preferred_element_type=F32
    )


def dot_t(left, right, precision=None):
    return lax.dot_general(
        left, right, (((1,), (1,)), ((), ())), precision=precision, preferred_element_type=F32
    )


def cholesky(gram):
    row = lax.broadcasted_iota(jnp.int32, (K, K), 0)
    col = lax.broadcasted_iota(jnp.int32, (K, K), 1)
    left = gram
    right = jnp.where(row == col, 1.0, 0.0).astype(F32)
    for k in range(0, K - 2, 2):
        first = jnp.broadcast_to(left[:, k : k + 1], (K, K))
        second = jnp.broadcast_to(left[:, k + 1 : k + 2], (K, K))
        a = first[k : k + 1, :]
        b = second[k : k + 1, :]
        d = second[k + 1 : k + 2, :]
        inverse = 1.0 / (a * d - b * b)
        below = row > k + 1
        of_first = jnp.where(below, first * (d * inverse) - second * (b * inverse), 0.0)
        of_second = jnp.where(below, second * (a * inverse) - first * (b * inverse), 0.0)
        left_k, left_l = left[k : k + 1, :], left[k + 1 : k + 2, :]
        right_k, right_l = right[k : k + 1, :], right[k + 1 : k + 2, :]
        left = left - of_first * left_k - of_second * left_l
        right = right - of_first * right_k - of_second * right_l
    odd = (row & 1) == 1
    pivots = jnp.sum(jnp.where(row == col, left, 0.0), axis=1, keepdims=True)
    beside = jnp.sum(jnp.where(row + 1 == col, left, 0.0), axis=1, keepdims=True)
    factor = jnp.where(odd, pltpu.roll(jnp.broadcast_to(beside / pivots, (K, K)), 1, 0), 0.0)
    left = left - factor * pltpu.roll(left, 1, 0)
    right = right - factor * pltpu.roll(right, 1, 0)
    pivots = jnp.sum(jnp.where(row == col, left, 0.0), axis=1, keepdims=True)
    scale = 1.0 / jnp.sqrt(pivots)
    return jnp.where(col >= row, left * scale, 0.0), jnp.where(col <= row, right * scale, 0.0)


def kernel(
    rows_hbm,
    cols_hbm,
    live_hbm,
    tiles_hbm,
    start_hbm,
    dual_hbm,
    proj_hbm,
    fact_hbm,
    next_hbm,
    rows_smem,
    cols_smem,
    live_smem,
    dual_ref,
    proj_ref,
    fact_ref,
    next_ref,
    gram_ref,
    start_gram,
    start_grams,
    slot_vmem,
    slot_ref,
    start_ref,
    tiles,
    cols_0,
    cols_1,
    cols_2,
    cols_3,
    cols_4,
    rows_0,
    rows_1,
    rows_2,
    rows_3,
    raw_x,
    basis,
    trans,
    products,
    pair_out,
    pair_in,
    back_out,
    back_in,
    own_back,
    own_direct,
    direct_out,
    direct_in,
    dots,
    load_sem,
    store_sem,
    slot_sem,
    tile_sem,
    pair_gram_send,
    pair_gram_recv,
    gram_send,
    gram_recv,
    cols_send,
    cols_recv,
    relay_send,
    relay_recv,
    rows_send,
    rows_recv,
    raw_send,
    raw_recv,
    dots_send,
    dots_recv,
    pair_send,
    pair_recv,
    back_send,
    back_recv,
    direct_send,
    direct_recv,
):
    cols_x = (cols_0, cols_1, cols_2, cols_3, cols_4)
    rows_x = (rows_0, rows_1, rows_2, rows_3)
    g = lax.axis_index("grp")
    r = lax.axis_index("row")
    core = lax.rem(r, 2)
    chip = lax.div(r, 2)
    z = lax.div(chip, SIDE)
    x = lax.rem(chip, SIDE)
    partner = r + 1 - 2 * core

    def chip_at(dz, dx):
        return lax.rem(z + dz, SIDE) * SIDE + lax.rem(x + dx, SIDE)

    def chip_from(dz, dx):
        return lax.rem(z + SIDE - dz, SIDE) * SIDE + lax.rem(x + SIDE - dx, SIDE)

    def remote(src, dst, send, recv, group, owner):
        return pltpu.make_async_remote_copy(
            src_ref=src,
            dst_ref=dst,
            send_sem=send,
            recv_sem=recv,
            device_id=(group, owner),
            device_id_type=MESH,
        )

    def await_recv(ref, send, recv):
        remote(ref, ref, send, recv, g, partner).wait_recv()

    def await_send(ref, send, recv):
        remote(ref, ref, send, recv, g, partner).wait_send()

    barrier = pltpu.get_barrier_semaphore()
    for dz, dx in FAR_FIRST:
        pl.semaphore_signal(
            barrier, inc=1, device_id=(g, chip_at(dz, dx) * 2 + core), device_id_type=MESH
        )
    for dy, dc in SMALL_GROUP:
        pl.semaphore_signal(
            barrier,
            inc=1,
            device_id=(lax.rem(g + dy, GRP), partner if dc else r),
            device_id_type=MESH,
        )

    loads = [
        pltpu.make_async_copy(src, dst, load_sem.at[i])
        for i, (src, dst) in enumerate(
            [
                (rows_hbm, rows_smem),
                (cols_hbm, cols_smem),
                (live_hbm, live_smem),
                (start_hbm, start_ref),
                (dual_hbm, dual_ref),
            ]
        )
    ]
    for copy in loads:
        copy.start()
    load = pltpu.make_async_copy(tiles_hbm, tiles, tile_sem)
    load.start()

    trans[...] = jnp.zeros_like(trans)
    products[TILES] = jnp.zeros((K, BS), F32)
    proj_ref[...] = jnp.zeros_like(proj_ref)
    for copy in loads:
        copy.wait()

    lane = lax.broadcasted_iota(jnp.int32, (1, GRP * ROW), 1)
    slots = jnp.full((1, GRP * ROW), TILES, jnp.int32)
    for k in range(TILES):
        place = jnp.where(live_smem[0, 0] > k, rows_smem[0, 0, k] * ROW + cols_smem[0, 0, k], -1)
        slots = jnp.where(lane == place, k, slots)
    slot_vmem[...] = slots
    table = pltpu.make_async_copy(slot_vmem, slot_ref, slot_sem)
    table.start()

    for i in range(GRP):
        block = start_ref[:, i * BS : (i + 1) * BS]
        high = block.astype(BF16)
        rows_0[i, 0:K, :] = high
        rows_0[i, K : 2 * K, :] = (block - high.astype(F32)).astype(BF16)
        raw_x[i, 0:K, :] = block
    cols_0[r] = rows_0[g]
    gram = dot_t(start_ref[...], start_ref[...], HIGHEST)
    for i in range(4):
        start_gram[core, :, i * K : (i + 1) * K] = gram[8 * i : 8 * i + 8]
    dual = dual_ref[:, pl.ds(pl.multiple_of(g * BS, BS), BS)]

    def send_cols(step):
        here = cols_x[step].at[r]
        for m, (dz, dx) in enumerate(FAR_FIRST):
            remote(
                here, here, cols_send.at[step], cols_recv.at[step, m], g, chip_at(dz, dx) * 2 + core
            ).start()
        if step < ITERS:
            remote(here, here, relay_send.at[step], relay_recv.at[step], g, partner).start()

    def receive_cols(step):
        for m in reversed(range(len(FAR_FIRST))):
            source = chip_from(*FAR_FIRST[m]) * 2 + core
            there = cols_x[step].at[source]
            await_recv(there, cols_send.at[step], cols_recv.at[step, m])
            if step < ITERS:
                remote(there, there, relay_send.at[step], relay_recv.at[step], g, partner).start()

    def products_of(load_left, rows, transposed):
        def body(k, carry):
            tile = tiles[k]
            product = dot_t(load_left(k), tile) if transposed else dot(load_left(k), tile)
            if rows == 2 * K:
                product = product[:K] + product[K:]
            products[k] = product
            return carry

        lax.fori_loop(0, TILES, body, 0, unroll=True)

    def back_sum(owner):
        total = products[slot_ref[0, owner]]
        for i in range(1, GRP):
            total = total + products[slot_ref[0, i * ROW + owner]]
        return total

    def send_pairs(step):
        def other(m, carry):
            pair_out[step, m] = back_sum(m * 2 + 1 - core).astype(BF16)
            return carry

        lax.fori_loop(0, CHIPS, other, 0, unroll=2)
        remote(
            pair_out.at[step],
            pair_in.at[step],
            pair_send.at[step],
            pair_recv.at[step],
            g,
            partner,
        ).start()

    def own_sums(step):
        def mine(m, carry):
            own_back[m] = back_sum(m * 2 + core)
            return carry

        lax.fori_loop(0, CHIPS, mine, 0, unroll=2)

    def send_back(step):
        with jax.named_scope("wait_pair"):
            await_recv(pair_in.at[step], pair_send.at[step], pair_recv.at[step])
        for dz, dx in FAR_FIRST:
            there = chip_at(dz, dx)
            back_out[step, there] = (
                own_back[there] + pair_in[step, there].astype(F32)
            ).astype(BF16)
        for dz, dx in FAR_FIRST:
            there = chip_at(dz, dx)
            remote(
                back_out.at[step, there],
                back_in.at[step, chip],
                back_send.at[step],
                back_recv.at[step],
                g,
                there * 2 + core,
            ).start()

    def send_direct(step):
        for dy in (2, 1, 3, 0):
            group = lax.rem(g + dy, GRP)

            def add(j, total, group=group):
                return total + products[slot_ref[0, group * ROW + j]]

            total = lax.fori_loop(0, ROW, add, jnp.zeros((K, BS), F32), unroll=8)
            if dy == 0:
                own_direct[...] = total
                continue
            direct_out[step, group] = total.astype(BF16)
            remote(
                direct_out.at[step, group],
                direct_in.at[step, g],
                direct_send.at[step],
                direct_recv.at[step],
                group,
                r,
            ).start()

    def send_start_gram():
        await_recv(start_gram.at[0], pair_gram_send, pair_gram_recv)
        start_grams[chip] = start_gram[0] + start_gram[1]
        mine = start_grams.at[chip]
        for dz, dx in FAR_FIRST:
            remote(mine, mine, gram_send, gram_recv, g, chip_at(dz, dx) * 2 + core).start()

    def receive_start_gram():
        await_recv(start_grams.at[pl.ds(0, CHIPS - 1)], gram_send, gram_recv)
        total = start_grams[0]
        for i in range(1, CHIPS):
            total = total + start_grams[i]
        return jnp.concatenate([total[:, i * K : (i + 1) * K] for i in range(4)], axis=0)

    def send_dots(step):
        width = K * step + 2 * K

        def add(p, total):
            owner = p * 2 + core
            so_far = jnp.concatenate([cols_x[s][owner] for s in range(step + 1)], axis=0)
            return total + dot_t(cols_x[step][owner], so_far)

        total = lax.fori_loop(0, CHIPS, add, jnp.zeros((K, width), F32), unroll=True)
        here = g * 2 + core
        dots[step, here, 0:K, 0:K] = total[:, 0:K] + total[:, K : 2 * K]
        if step > 1:
            dots[step, here, 0:K, K : K * step] = total[:, 2 * K : K + K * step]
        gram = total[:, K + K * step :]
        if step < ITERS:
            dots[step, here, 0:K, K * step : K + K * step] = gram
        else:
            for i in range(4):
                dots[step, here, K:, i * K : (i + 1) * K] = gram[8 * i : 8 * i + 8]
        mine = dots.at[step, here, pl.ds(0, dots_height(step))]
        for dy, dc in SMALL_GROUP:
            remote(
                mine,
                mine,
                dots_send.at[step],
                dots_recv.at[step],
                lax.rem(g + dy, GRP),
                partner if dc else r,
            ).start()

    def receive_dots(step):
        with jax.named_scope("wait_dots"):
            await_recv(
                dots.at[step, pl.ds(0, 7), pl.ds(0, dots_height(step))],
                dots_send.at[step],
                dots_recv.at[step],
            )
        total = dots[step, 0, 0 : dots_height(step)]
        for i in range(1, 2 * GRP):
            total = total + dots[step, i, 0 : dots_height(step)]
        if step < ITERS:
            gram = total[:, K * step : K + K * step]
        else:
            gram = jnp.concatenate([total[K:, i * K : (i + 1) * K] for i in range(4)], axis=0)
        coef = dot_t(total[0:K, : K * step], trans[0 : K * step, 0 : K * step], HIGHEST)
        if step > 1:
            coef = dot(inverses[step - 1], coef, HIGHEST)
            gram = dot_t(dot(inverses[step - 1], gram, HIGHEST), inverses[step - 1], HIGHEST)
        gram_ref[...] = gram - dot_t(coef, coef, HIGHEST)
        return coef, gram_ref[...]

    def normalise(step, coef, gram):
        with jax.named_scope("cholesky"):
            upper, inverse = cholesky(gram)
        own = inverse if step < 2 else dot(inverse, inverses[step - 1], HIGHEST)
        trans[K * step : K + K * step, K * step : K + K * step] = own
        if step > 0:
            fact_ref[step - 1] = upper.T
            trans[K * step : K + K * step, 0 : K * step] = -dot(
                inverse,
                dot(coef, trans[0 : K * step, 0 : K * step], HIGHEST),
                HIGHEST,
            )
        uppers[step] = upper
        inverses[step] = inverse

    def record(step, coef):
        row = lax.broadcasted_iota(jnp.int32, (K, K), 0)
        col = lax.broadcasted_iota(jnp.int32, (K, K), 1)
        at = K * (step - 1)
        if step > 1:
            if step > 2:
                proj_ref[step - 1, :, 0 : at - K] = coef[:, : at - K]
            proj_ref[step - 1, :, at - K : at] = coef[:, at - K : at] + uppers[step - 1]
        proj_ref[step - 1, :, at : at + K] = coef[:, at:] + jnp.where(row == col, SHIFT, 0.0)

    stores = [
        pltpu.make_async_copy(src, dst, store_sem.at[i])
        for i, (src, dst) in enumerate(
            [(proj_ref, proj_hbm), (fact_ref, fact_hbm), (next_ref, next_hbm)]
        )
    ]
    uppers = {}
    inverses = {}
    scope = jax.named_scope
    ahead = None
    for step in range(ITERS):
        size = height(step)
        if ahead is not None:
            ahead()
        if step == 0:
            with scope("load"):
                load.wait()
                table.wait()
            with scope("back"):
                products_of(lambda k: rows_0[rows_smem[0, 0, k]], size, False)
            with scope("enter"):
                pl.semaphore_wait(barrier, len(FAR_FIRST) + len(SMALL_GROUP))
            mine = start_gram.at[core]
            remote(mine, mine, pair_gram_send, pair_gram_recv, g, partner).start()
            send_cols(0)
        else:
            with scope("wait_rows"):
                await_recv(rows_x[step].at[pl.ds(0, 3)], rows_send.at[step], rows_recv.at[step])
            with scope("back"):
                products_of(lambda k, step=step: rows_x[step][rows_smem[0, 0, k]], size, False)
        with scope("pairs"):
            send_pairs(step)
        with scope("own_sums"):
            own_sums(step)
            if step == 0:
                send_start_gram()
        with scope("wait_cols"):
            receive_cols(step)
        with scope("send_back"):
            send_back(step)
        if step > 0:
            with scope("dots"):
                send_dots(step)
        with scope("wait_relay"):
            await_recv(cols_x[step].at[pl.ds(0, CHIPS)], relay_send.at[step], relay_recv.at[step])
        with scope("forward"):
            products_of(lambda k, step=step: cols_x[step][cols_smem[0, 0, k]], size, True)
        with scope("direct"):
            send_direct(step)

        if step == 0:
            with scope("wait_dots"):
                coef, gram = None, receive_start_gram()
            normalise(0, None, gram)
            scaled = dot(inverses[0], raw_x[g, 0:K, :], HIGHEST)
            known = scaled * (-SHIFT)
            basis[0:K, 0:BS] = scaled
        else:
            coef, gram = receive_dots(step)
            with scope("known"):
                block = raw_x[g, K * step : K * step + K, :]
                if step > 1:
                    block = dot(inverses[step - 1], block, HIGHEST)
                in_basis = dot(coef, basis[0 : K * step, :], HIGHEST)
                block = block - in_basis[:, :BS]
                known = (
                    block * (-SHIFT)
                    - in_basis[:, BS:]
                    - dot(gram, basis[K * (step - 1) : K * step, 0:BS], HIGHEST)
                )

        with scope("wait_direct"):
            await_recv(
                direct_in.at[step, pl.ds(0, 3)], direct_send.at[step], direct_recv.at[step]
            )
        with scope("wait_back"):
            await_recv(
                back_in.at[step, pl.ds(0, CHIPS - 1)], back_send.at[step], back_recv.at[step]
            )
        with scope("update"):
            total = own_direct[...]
            for dy in (1, 2, 3):
                total = total + direct_in[step, lax.rem(g + dy, GRP)].astype(F32)
            total = total + own_back[chip] + pair_in[step, chip].astype(F32)
            for dz, dx in FAR_FIRST:
                total = total + back_in[step, chip_at(dz, dx)].astype(F32)
            image = 0.5 * total - raw_x[g, K * step : K * step + K, :] * dual
            if step == 0:
                image = dot(inverses[0], image, HIGHEST)
                basis[0:K, BS:] = image
                following = image + known
            else:
                if step > 1:
                    image = dot(inverses[step - 1], image, HIGHEST)
                following = image + known
                image = image - in_basis[:, BS:]
            rounded = following.astype(BF16)
            after = step + 1
            cols_x[after][r] = rounded
            raw_x[g, K * after : K * after + K, :] = following
            if after < ITERS:
                rows_x[after][g] = rounded
                mine = rows_x[after].at[g]
                for dy in (2, 1, 3):
                    remote(
                        mine,
                        mine,
                        rows_send.at[after],
                        rows_recv.at[after],
                        lax.rem(g + dy, GRP),
                        r,
                    ).start()
            send_cols(after)
            mine = raw_x.at[g, pl.ds(K * after, K), :]
            for dy in (2, 1, 3):
                remote(
                    mine, mine, raw_send.at[after], raw_recv.at[after], lax.rem(g + dy, GRP), r
                ).start()

        def ahead(step=step, coef=coef, gram=gram, block=None if step == 0 else block, image=image):
            if step > 0:
                normalise(step, coef, gram)
                at = K * step
                basis[at : at + K, 0:BS] = dot(inverses[step], block, HIGHEST)
                basis[at : at + K, BS:] = dot(inverses[step], image, HIGHEST)
                record(step, coef)

    ahead()
    with scope("wait_cols"):
        receive_cols(ITERS)
    with scope("dots"):
        send_dots(ITERS)
    coef, gram = receive_dots(ITERS)
    normalise(ITERS, coef, gram)
    with scope("final"):
        record(ITERS, coef)
        for step in range(1, ITERS + 1):
            await_recv(
                raw_x.at[pl.ds(0, 3), pl.ds(K * step, K), :], raw_send.at[step], raw_recv.at[step]
            )
        final = trans[K * ITERS : K * ITERS + K, :]
        for copy in stores[:2]:
            copy.start()
        for i in range(GRP):
            next_ref[:, i * BS : (i + 1) * BS] = dot(final, raw_x[i], HIGHEST)

    stores[2].start()
    await_send(start_gram.at[0], pair_gram_send, pair_gram_recv)
    await_send(start_grams.at[pl.ds(0, CHIPS - 1)], gram_send, gram_recv)
    for step in range(ITERS + 1):
        await_send(cols_x[step].at[pl.ds(0, CHIPS - 1)], cols_send.at[step], cols_recv.at[step, 0])
        if step > 0:
            await_send(
                dots.at[step, pl.ds(0, 7), pl.ds(0, dots_height(step))],
                dots_send.at[step],
                dots_recv.at[step],
            )
        if step > 0:
            await_send(
                raw_x.at[pl.ds(0, 3), pl.ds(K * step, K), :], raw_send.at[step], raw_recv.at[step]
            )
        if step == ITERS:
            continue
        await_send(cols_x[step].at[pl.ds(0, CHIPS)], relay_send.at[step], relay_recv.at[step])
        await_send(pair_out.at[step], pair_send.at[step], pair_recv.at[step])
        await_send(back_in.at[step, pl.ds(0, CHIPS - 1)], back_send.at[step], back_recv.at[step])
        await_send(direct_in.at[step, pl.ds(0, 3)], direct_send.at[step], direct_recv.at[step])
        if step > 0:
            await_send(rows_x[step].at[pl.ds(0, 3)], rows_send.at[step], rows_recv.at[step])
    for copy in stores:
        copy.wait()


def write_out(*refs):
    inputs, outputs, held, sems = refs[:3], refs[3:6], refs[6:9], refs[9]
    reads = [pltpu.make_async_copy(inputs[i], held[i], sems.at[0, i]) for i in range(3)]
    writes = [pltpu.make_async_copy(held[i], outputs[i], sems.at[1, i]) for i in range(3)]
    for copy in reads:
        copy.start()
    for i in range(3):
        reads[i].wait()
        writes[i].start()
    for copy in writes:
        copy.wait()


def per_device(tiles, tile_rows, tile_cols, live_tiles, dual_shift, start_block):
    hbm = pl.BlockSpec(memory_space=pltpu.HBM)
    dma = pltpu.SemaphoreType.DMA
    steps = ITERS + 1
    out = pl.pallas_call(
        kernel,
        out_shape=(
            jax.ShapeDtypeStruct((ITERS, K, ITERS * K), F32),
            jax.ShapeDtypeStruct((ITERS, K, K), F32),
            jax.ShapeDtypeStruct((K, GRP * BS), F32),
        ),
        in_specs=[hbm] * 6,
        out_specs=(hbm, hbm, hbm),
        scratch_shapes=[
            pltpu.SMEM((1, 1, TILES), jnp.int32),
            pltpu.SMEM((1, 1, TILES), jnp.int32),
            pltpu.SMEM((1, 1), jnp.int32),
            pltpu.VMEM((1, GRP * BS), F32),
            pltpu.VMEM((ITERS, K, ITERS * K), F32),
            pltpu.VMEM((ITERS, K, K), F32),
            pltpu.VMEM((K, GRP * BS), F32),
            pltpu.VMEM((K, K), F32),
            pltpu.VMEM((2, 8, 128), F32),
            pltpu.VMEM((CHIPS, 8, 128), F32),
            pltpu.VMEM((1, GRP * ROW), jnp.int32),
            pltpu.SMEM((1, GRP * ROW), jnp.int32),
            pltpu.VMEM((K, GRP * BS), F32),
            pltpu.VMEM((TILES, BS, BS), BF16),
            *[pltpu.VMEM((ROW, height(step), BS), BF16) for step in range(steps)],
            *[pltpu.VMEM((GRP, height(step), BS), BF16) for step in range(ITERS)],
            pltpu.VMEM((GRP, K * steps, BS), F32),
            pltpu.VMEM((K * ITERS, 2 * BS), F32),
            pltpu.VMEM((K * steps, K * steps), F32),
            pltpu.VMEM((TILES + 1, K, BS), F32),
            pltpu.VMEM((ITERS, CHIPS, K, BS), BF16),
            pltpu.VMEM((ITERS, CHIPS, K, BS), BF16),
            pltpu.VMEM((ITERS, CHIPS, K, BS), BF16),
            pltpu.VMEM((ITERS, CHIPS, K, BS), BF16),
            pltpu.VMEM((CHIPS, K, BS), F32),
            pltpu.VMEM((K, BS), F32),
            pltpu.VMEM((ITERS, GRP, K, BS), BF16),
            pltpu.VMEM((ITERS, GRP, K, BS), BF16),
            pltpu.VMEM((steps, 2 * GRP, K + 8, 128), F32),
            dma((5,)),
            dma((3,)),
            dma,
            dma,
            dma,
            dma,
            dma,
            dma,
            dma((steps,)),
            dma((steps, CHIPS - 1)),
            dma((ITERS,)),
            dma((ITERS,)),
            dma((ITERS,)),
            dma((ITERS,)),
            dma((steps,)),
            dma((steps,)),
            dma((steps,)),
            dma((steps,)),
            dma((ITERS,)),
            dma((ITERS,)),
            dma((ITERS,)),
            dma((ITERS,)),
            dma((ITERS,)),
            dma((ITERS,)),
        ],
        compiler_params=pltpu.CompilerParams(
            collective_id=0, has_side_effects=True, vmem_limit_bytes=60 * 1024 * 1024
        ),
        name="lanczos",
    )(
        tile_rows,
        tile_cols,
        live_tiles,
        tiles.reshape(TILES, BS, BS),
        start_block,
        dual_shift.reshape(1, GRP * BS),
    )
    return pl.pallas_call(
        write_out,
        out_shape=tuple(jax.ShapeDtypeStruct(a.shape, a.dtype) for a in out),
        in_specs=[hbm] * 3,
        out_specs=(hbm, hbm, hbm),
        scratch_shapes=[*[pltpu.VMEM(a.shape, a.dtype) for a in out], dma((2, 3))],
        compiler_params=pltpu.CompilerParams(vmem_limit_bytes=60 * 1024 * 1024),
        name="write_out",
    )(*out)


def solution(mesh):
    in_specs = (
        P("grp", "row", None, None, None),
        P("grp", "row", None),
        P("grp", "row", None),
        P("grp", "row"),
        P("row"),
        P(None, "row"),
    )
    out_specs = (P(), P(), P(None, "row"))
    return jax.shard_map(
        per_device, mesh=mesh, in_specs=in_specs, out_specs=out_specs, check_vma=False
    )
```

```python
import contextlib
import functools

import jax
import jax.numpy as jnp
from jax import lax
from jax.experimental import pallas as pl
from jax.experimental.pallas import tpu as pltpu
from jax.sharding import PartitionSpec as P

MESH = pl.DeviceIdType.MESH
HIGHEST = lax.Precision.HIGHEST
F32 = jnp.float32
BF16 = jnp.bfloat16

ITERS = 4
K = 32
BS = 256
GRP = 4
ROW = 32
CHIPS = ROW // 2
SIDE = 4
TILES = 32
WAVES = (5, 5, 3, 2)
PARTS = 4
SHIFT = -1.0

FAR_FIRST = sorted(
    [(dz, dx) for dz in range(SIDE) for dx in range(SIDE) if (dz, dx) != (0, 0)],
    key=lambda d: -(min(d[0], SIDE - d[0]) + min(d[1], SIDE - d[1])),
)
SMALL_GROUP = [(dy, dc) for dy in (2, 1, 3, 0) for dc in (1, 0) if (dy, dc) != (0, 0)]


def height(step):
    return 2 * K if step == 0 else K


@contextlib.contextmanager
def phase(name):
    with jax.named_scope(name):
        yield
    if name in ("update", "cholesky", "dots", "direct", "pairs"):
        pl.delay(1)


def wave_of(m):
    return next(w for w in range(len(WAVES)) if m < sum(WAVES[: w + 1]))


def dots_height(step):
    return K if step < ITERS else K + 8


def dot(left, right, precision=None):
    return lax.dot_general(
        left, right, (((1,), (0,)), ((), ())), precision=precision, preferred_element_type=F32
    )


def t_dot(left, right, precision=None):
    return lax.dot_general(
        left, right, (((0,), (0,)), ((), ())), precision=precision, preferred_element_type=F32
    )


def dot_t(left, right, precision=None):
    return lax.dot_general(
        left, right, (((1,), (1,)), ((), ())), precision=precision, preferred_element_type=F32
    )


def cholesky(gram):
    row = lax.broadcasted_iota(jnp.int32, (K, K), 0)
    col = lax.broadcasted_iota(jnp.int32, (K, K), 1)
    left = gram
    right = jnp.where(row == col, 1.0, 0.0).astype(F32)
    for k in range(0, K - 2, 2):
        first = jnp.broadcast_to(left[:, k : k + 1], (K, K))
        second = jnp.broadcast_to(left[:, k + 1 : k + 2], (K, K))
        a = first[k : k + 1, :]
        b = second[k : k + 1, :]
        d = second[k + 1 : k + 2, :]
        inverse = 1.0 / (a * d - b * b)
        below = row > k + 1
        of_first = jnp.where(below, first * (d * inverse) - second * (b * inverse), 0.0)
        of_second = jnp.where(below, second * (a * inverse) - first * (b * inverse), 0.0)
        left_k, left_l = left[k : k + 1, :], left[k + 1 : k + 2, :]
        right_k, right_l = right[k : k + 1, :], right[k + 1 : k + 2, :]
        left = left - of_first * left_k - of_second * left_l
        right = right - of_first * right_k - of_second * right_l
    odd = (row & 1) == 1
    pivots = jnp.sum(jnp.where(row == col, left, 0.0), axis=1, keepdims=True)
    beside = jnp.sum(jnp.where(row + 1 == col, left, 0.0), axis=1, keepdims=True)
    factor = jnp.where(odd, pltpu.roll(jnp.broadcast_to(beside / pivots, (K, K)), 1, 0), 0.0)
    left = left - factor * pltpu.roll(left, 1, 0)
    right = right - factor * pltpu.roll(right, 1, 0)
    pivots = jnp.sum(jnp.where(row == col, left, 0.0), axis=1, keepdims=True)
    scale = 1.0 / jnp.sqrt(pivots)
    return jnp.where(col >= row, left * scale, 0.0), jnp.where(col <= row, right * scale, 0.0)


def kernel(
    rows_hbm,
    cols_hbm,
    live_hbm,
    tiles_hbm,
    start_hbm,
    dual_hbm,
    proj_ref,
    fact_ref,
    next_ref,
    rows_smem,
    cols_smem,
    live_smem,
    dual_ref,
    gram_ref,
    start_gram,
    start_grams,
    slot_vmem,
    slot_ref,
    start_ref,
    tiles,
    turned,
    cols_0,
    cols_1,
    cols_2,
    cols_3,
    rows_0,
    rows_1,
    rows_2,
    rows_3,
    raw_x,
    basis,
    in_blocks,
    old_rows,
    trans,
    products,
    pair_out,
    pair_in,
    back_out,
    back_in,
    own_back,
    own_direct,
    direct_out,
    direct_in,
    dots,
    last,
    load_sem,
    slot_sem,
    tile_sem,
    pair_gram_send,
    pair_gram_recv,
    gram_send,
    gram_recv,
    last_send,
    last_recv,
    cols_send,
    cols_recv,
    relay_send,
    relay_recv,
    rows_send,
    rows_recv,
    raw_send,
    raw_recv,
    dots_send,
    dots_recv,
    pair_send,
    pair_recv,
    back_send,
    back_recv,
    direct_send,
    direct_recv,
):
    cols_x = (cols_0, cols_1, cols_2, cols_3)
    rows_x = (rows_0, rows_1, rows_2, rows_3)
    g = lax.axis_index("grp")
    r = lax.axis_index("row")
    core = lax.rem(r, 2)
    chip = lax.div(r, 2)
    z = lax.div(chip, SIDE)
    x = lax.rem(chip, SIDE)
    partner = r + 1 - 2 * core

    def chip_at(dz, dx):
        return lax.rem(z + dz, SIDE) * SIDE + lax.rem(x + dx, SIDE)

    def chip_from(dz, dx):
        return lax.rem(z + SIDE - dz, SIDE) * SIDE + lax.rem(x + SIDE - dx, SIDE)

    def remote(src, dst, send, recv, group, owner):
        return pltpu.make_async_remote_copy(
            src_ref=src,
            dst_ref=dst,
            send_sem=send,
            recv_sem=recv,
            device_id=(group, owner),
            device_id_type=MESH,
        )

    def await_recv(ref, send, recv):
        remote(ref, ref, send, recv, g, partner).wait_recv()

    def await_send(ref, send, recv):
        remote(ref, ref, send, recv, g, partner).wait_send()

    barrier = pltpu.get_barrier_semaphore()
    for dz, dx in FAR_FIRST:
        pl.semaphore_signal(
            barrier, inc=1, device_id=(g, chip_at(dz, dx) * 2 + core), device_id_type=MESH
        )
    for dy, dc in SMALL_GROUP:
        pl.semaphore_signal(
            barrier,
            inc=1,
            device_id=(lax.rem(g + dy, GRP), partner if dc else r),
            device_id_type=MESH,
        )

    loads = [
        pltpu.make_async_copy(src, dst, load_sem.at[i])
        for i, (src, dst) in enumerate(
            [
                (rows_hbm, rows_smem),
                (cols_hbm, cols_smem),
                (live_hbm, live_smem),
                (start_hbm, start_ref),
                (dual_hbm, dual_ref),
            ]
        )
    ]
    for copy in loads:
        copy.start()
    load = pltpu.make_async_copy(tiles_hbm, tiles, tile_sem)
    load.start()

    trans[...] = jnp.zeros_like(trans)
    products[TILES] = jnp.zeros((K, BS), F32)
    proj_ref[...] = jnp.zeros_like(proj_ref)
    for copy in loads:
        copy.wait()

    lane = lax.broadcasted_iota(jnp.int32, (1, GRP * ROW), 1)
    slots = jnp.full((1, GRP * ROW), TILES, jnp.int32)
    for k in range(TILES):
        place = jnp.where(live_smem[0, 0] > k, rows_smem[0, 0, k] * ROW + cols_smem[0, 0, k], -1)
        slots = jnp.where(lane == place, k, slots)
    slot_vmem[...] = slots
    table = pltpu.make_async_copy(slot_vmem, slot_ref, slot_sem)
    table.start()

    for i in range(GRP):
        block = start_ref[:, i * BS : (i + 1) * BS]
        high = block.astype(BF16)
        rows_0[i, 0:K, :] = high
        rows_0[i, K : 2 * K, :] = (block - high.astype(F32)).astype(BF16)
        raw_x[i, 0:K, :] = block
    cols_0[r] = rows_0[g]
    gram = dot_t(start_ref[...], start_ref[...], HIGHEST)
    for i in range(4):
        start_gram[core, :, i * K : (i + 1) * K] = gram[8 * i : 8 * i + 8]
    dual = dual_ref[:, pl.ds(pl.multiple_of(g * BS, BS), BS)]

    def send_cols(step):
        here = cols_x[step].at[r]
        for m, (dz, dx) in enumerate(FAR_FIRST):
            remote(
                here, here, cols_send, cols_recv.at[step % 2, wave_of(m)], g, chip_at(dz, dx) * 2 + core
            ).start()
        remote(here, here, relay_send, relay_recv.at[step % 2], g, partner).start()

    def receive_cols(step):
        first = 0
        for wave, count in enumerate(WAVES):
            await_recv(
                cols_x[step].at[pl.ds(0, count)], cols_send, cols_recv.at[step % 2, wave]
            )
            for m in range(first, first + count):
                there = cols_x[step].at[chip_from(*FAR_FIRST[m]) * 2 + core]
                remote(there, there, relay_send, relay_recv.at[step % 2], g, partner).start()
            first += count

    def sent(step):
        await_send(cols_x[step].at[pl.ds(0, CHIPS - 1)], cols_send, cols_recv.at[0, 0])
        await_send(cols_x[step].at[pl.ds(0, CHIPS)], relay_send, relay_recv.at[0])
        await_send(pair_out.at[step], pair_send, pair_recv.at[0])
        await_send(back_in.at[step, pl.ds(0, CHIPS - 1)], back_send, back_recv.at[0])
        await_send(direct_in.at[step, pl.ds(0, 3)], direct_send, direct_recv.at[0])
        if step > 0:
            await_send(rows_x[step].at[pl.ds(0, 3)], rows_send, rows_recv.at[0])
            await_send(dots.at[step, pl.ds(0, 7), pl.ds(0, K)], dots_send, dots_recv.at[0])

    def send_raw(step):
        if step > 1:
            receive_raw(step - 1)
        mine = raw_x.at[g, pl.ds(K * step, K), :]
        for dy in (2, 1, 3):
            remote(
                mine, mine, raw_send, raw_recv.at[step % 2], lax.rem(g + dy, GRP), r
            ).start()

    def receive_raw(step):
        others = raw_x.at[pl.ds(0, 3), pl.ds(K * step, K), :]
        await_recv(others, raw_send, raw_recv.at[step % 2])
        await_send(others, raw_send, raw_recv.at[step % 2])

    def products_of(load_left, rows, matrices):
        def body(k, carry):
            product = dot(load_left(k), matrices[k])
            if rows == 2 * K:
                product = product[:K] + product[K:]
            products[k] = product
            return carry

        lax.fori_loop(0, TILES, body, 0, unroll=True)

    def back_sum(owner):
        total = products[slot_ref[0, owner]]
        for i in range(1, GRP):
            total = total + products[slot_ref[0, i * ROW + owner]]
        return total

    def send_pairs(step):
        for part in range(PARTS):

            def other(m, carry):
                pair_out[step, m] = back_sum(m * 2 + 1 - core).astype(BF16)
                return carry

            size = CHIPS // PARTS
            lax.fori_loop(part * size, part * size + size, other, 0, unroll=2)
            here = pl.ds(part * size, size)
            remote(
                pair_out.at[step, here],
                pair_in.at[step, here],
                pair_send,
                pair_recv.at[step % 2],
                g,
                partner,
            ).start()

    def own_sums(step):
        def mine(m, carry):
            own_back[m] = back_sum(m * 2 + core)
            return carry

        lax.fori_loop(0, CHIPS, mine, 0, unroll=2)

    def send_back(step):
        with phase("wait_pair"):
            await_recv(pair_in.at[step], pair_send, pair_recv.at[step % 2])
        for dz, dx in FAR_FIRST:
            there = chip_at(dz, dx)
            back_out[step, there] = (
                own_back[there] + pair_in[step, there].astype(F32)
            ).astype(BF16)
        for dz, dx in FAR_FIRST:
            there = chip_at(dz, dx)
            remote(
                back_out.at[step, there],
                back_in.at[step, chip],
                back_send,
                back_recv.at[step % 2],
                g,
                there * 2 + core,
            ).start()

    def send_direct(step):
        for dy in (2, 1, 3, 0):
            group = lax.rem(g + dy, GRP)

            def add(j, total, group=group):
                return total + products[slot_ref[0, group * ROW + j]]

            total = lax.fori_loop(0, ROW, add, jnp.zeros((K, BS), F32), unroll=8)
            if dy == 0:
                own_direct[...] = total
                continue
            direct_out[step, group] = total.astype(BF16)
            remote(
                direct_out.at[step, group],
                direct_in.at[step, g],
                direct_send,
                direct_recv.at[step % 2],
                group,
                r,
            ).start()

    def send_start_gram():
        await_recv(start_gram.at[0], pair_gram_send, pair_gram_recv)
        start_grams[chip] = start_gram[0] + start_gram[1]
        mine = start_grams.at[chip]
        for dz, dx in FAR_FIRST:
            remote(mine, mine, gram_send, gram_recv, g, chip_at(dz, dx) * 2 + core).start()

    def receive_start_gram():
        await_recv(start_grams.at[pl.ds(0, CHIPS - 1)], gram_send, gram_recv)
        total = start_grams[0]
        for i in range(1, CHIPS):
            total = total + start_grams[i]
        return jnp.concatenate([total[:, i * K : (i + 1) * K] for i in range(4)], axis=0)

    def send_dots(step):
        width = K * step + K

        totals = [jnp.zeros((K, width), F32) for _ in range(4)]
        for p in range(CHIPS):
            owner = p * 2 + core
            so_far = jnp.concatenate([cols_x[s][owner, 0:K] for s in range(step + 1)], axis=0)
            totals[p % 4] = totals[p % 4] + dot_t(cols_x[step][owner], so_far)
        total = (totals[0] + totals[1]) + (totals[2] + totals[3])
        here = g * 2 + core
        dots[step, here, 0:K, 0:width] = total
        spread_dots(step)

    def spread_dots(step):
        here = g * 2 + core
        mine = dots.at[step, here, pl.ds(0, dots_height(step))]
        for dy, dc in SMALL_GROUP:
            remote(
                mine,
                mine,
                dots_send,
                dots_recv.at[step % 2],
                lax.rem(g + dy, GRP),
                partner if dc else r,
            ).start()

    def send_last():
        block = raw_x[g, K * ITERS :, :]
        last[chip, 0:K, :] = dot_t(block, raw_x[g, 0 : K * ITERS, :], HIGHEST)
        gram = dot_t(block, block, HIGHEST)
        for i in range(4):
            last[chip, K:, i * K : (i + 1) * K] = gram[8 * i : 8 * i + 8]
        mine = last.at[chip]
        for dz, dx in FAR_FIRST:
            remote(mine, mine, last_send, last_recv, g, chip_at(dz, dx) * 2 + core).start()

    def spread_last():
        await_recv(last.at[pl.ds(0, CHIPS - 1)], last_send, last_recv)
        total = last[0]
        for i in range(1, CHIPS):
            total = total + last[i]
        dots[ITERS, g * 2 + core] = total
        spread_dots(ITERS)

    def receive_dots(step):
        with phase("wait_dots"):
            await_recv(
                dots.at[step, pl.ds(0, 7), pl.ds(0, dots_height(step))],
                dots_send,
                dots_recv.at[step % 2],
            )
        total = dots[step, 0, 0 : dots_height(step)]
        for i in range(1, 2 * GRP):
            total = total + dots[step, i, 0 : dots_height(step)]
        if step < ITERS:
            gram = total[:, K * step : K + K * step]
        else:
            gram = jnp.concatenate([total[K:, i * K : (i + 1) * K] for i in range(4)], axis=0)
        products_before = total[0:K, : K * step]
        coef = dot_t(products_before, trans[0 : K * step, 0 : K * step], HIGHEST)
        return products_before, coef, gram - dot_t(coef, coef, HIGHEST)

    def scaled(step, coef, gram):
        if step > 1:
            coef = dot(inverses[step - 1], coef, HIGHEST)
            gram = dot_t(dot(inverses[step - 1], gram, HIGHEST), inverses[step - 1], HIGHEST)
        gram_ref[...] = gram
        return coef, gram_ref[...]

    def normalise(step, coef, gram):
        with phase("cholesky"):
            upper, inverse = cholesky(gram)
        if step > 0:
            fact_ref[step - 1] = upper.T
        if step < ITERS:
            own = inverse if step < 2 else dot(inverse, inverses[step - 1], HIGHEST)
            trans[K * step : K + K * step, K * step : K + K * step] = own
            if step > 0:
                trans[K * step : K + K * step, 0 : K * step] = -dot(
                    inverse,
                    dot(coef, trans[0 : K * step, 0 : K * step], HIGHEST),
                    HIGHEST,
                )
        uppers[step] = upper
        inverses[step] = inverse

    def record(step, coef):
        row = lax.broadcasted_iota(jnp.int32, (K, K), 0)
        col = lax.broadcasted_iota(jnp.int32, (K, K), 1)
        at = K * (step - 1)
        if step > 1:
            if step > 2:
                proj_ref[step - 1, :, 0 : at - K] = coef[:, : at - K]
            proj_ref[step - 1, :, at - K : at] = coef[:, at - K : at] + uppers[step - 1]
        proj_ref[step - 1, :, at : at + K] = coef[:, at:] + jnp.where(row == col, SHIFT, 0.0)

    uppers = {}
    inverses = {}
    scope = phase
    ahead = None
    for step in range(ITERS):
        size = height(step)
        if ahead is not None:
            newest = ahead()
        if step == 0:
            with scope("enter"):
                pl.semaphore_wait(barrier, len(FAR_FIRST) + len(SMALL_GROUP))
            mine = start_gram.at[core]
            remote(mine, mine, pair_gram_send, pair_gram_recv, g, partner).start()
            send_cols(0)
            with scope("load"):
                load.wait()
                table.wait()
            with scope("back"):
                products_of(lambda k: rows_0[rows_smem[0, 0, k]], size, tiles)
        else:
            with scope("wait_rows"):
                await_recv(rows_x[step].at[pl.ds(0, 3)], rows_send, rows_recv.at[step % 2])
            send_raw(step)
            with scope("back"):
                products_of(lambda k, step=step: rows_x[step][rows_smem[0, 0, k]], size, tiles)
        with scope("pairs"):
            send_pairs(step)
        with scope("own_sums"):
            own_sums(step)
            if step == 0:
                send_start_gram()
        if step == 0:
            with scope("turn"):

                def turn(k, carry):
                    turned[k] = tiles[k].T
                    return carry

                lax.fori_loop(0, TILES, turn, 0, unroll=2)

        @pl.when(core == 0)
        def _(step=step):
            send_back(step)

        with scope("wait_cols"):
            receive_cols(step)
        if step > 0:
            with scope("dots"):
                send_dots(step)

        @pl.when(core == 1)
        def _(step=step):
            send_back(step)

        with scope("wait_relay"):
            await_recv(cols_x[step].at[pl.ds(0, CHIPS)], relay_send, relay_recv.at[step % 2])
        with scope("forward"):
            products_of(lambda k, step=step: cols_x[step][cols_smem[0, 0, k]], size, turned)
        with scope("direct"):
            send_direct(step)

        if step == 0:
            with scope("wait_dots"):
                coef, gram = None, receive_start_gram()
            normalise(0, None, gram)
            first = dot(inverses[0], raw_x[g, 0:K, :], HIGHEST)
            known = first * (-SHIFT)
            basis[0:K, 0:BS] = first
        else:
            before, coef, gram = receive_dots(step)
            with scope("known"):
                known = raw_x[g, K * step : K * step + K, :] * (-SHIFT)
                known = known - dot(before, in_blocks[0 : K * step, :], HIGHEST)
                known = known - dot(gram, newest, HIGHEST)

        with scope("wait_direct"):
            await_recv(
                direct_in.at[step, pl.ds(0, 3)], direct_send, direct_recv.at[step % 2]
            )
        with scope("wait_back"):
            await_recv(
                back_in.at[step, pl.ds(0, CHIPS - 1)], back_send, back_recv.at[step % 2]
            )
        with scope("update"):
            total = own_direct[...]
            for dy in (1, 2, 3):
                total = total + direct_in[step, lax.rem(g + dy, GRP)].astype(F32)
            total = total + own_back[chip] + pair_in[step, chip].astype(F32)
            for dz, dx in FAR_FIRST:
                total = total + back_in[step, chip_at(dz, dx)].astype(F32)
            image = 0.5 * total - raw_x[g, K * step : K * step + K, :] * dual
            if step == 0:
                image = dot(inverses[0], image, HIGHEST)
                basis[0:K, BS:] = image
                following = image + known
            elif step == 1:
                following = image + known
            else:
                following = dot(inverses[step - 1], image + known, HIGHEST)
            sent(step)
            rounded = following.astype(BF16)
            after = step + 1
            raw_x[g, K * after : K * after + K, :] = following
            if after < ITERS:
                cols_x[after][r] = rounded
                rows_x[after][g] = rounded
                mine = rows_x[after].at[g]
                for dy in (2, 1, 3):
                    remote(
                        mine,
                        mine,
                        rows_send,
                        rows_recv.at[after % 2],
                        lax.rem(g + dy, GRP),
                        r,
                    ).start()
                send_cols(after)
            else:
                send_last()
                send_raw(after)

        def ahead(step=step, coef=coef, gram=gram, image=image):
            at = K * step
            if step > 0:
                coef, gram = scaled(step, coef, gram)
                normalise(step, coef, gram)
                both = jnp.concatenate([raw_x[g, at : at + K, :], image], axis=1)
                if step > 1:
                    both = dot(inverses[step - 1], both, HIGHEST)
                both = both - dot(coef, basis[0:at, :], HIGHEST)
                basis[at : at + K, :] = dot(inverses[step], both, HIGHEST)
                record(step, coef)
            if step == ITERS - 1:
                return None
            size = at + K
            in_blocks[0:size, :] = t_dot(
                trans[0:size, 0:size],
                basis[0:size, BS:] - SHIFT * basis[0:size, 0:BS],
                HIGHEST,
            )
            last = basis[at : at + K, 0:BS]
            return last if step == 0 else t_dot(inverses[step], last, HIGHEST)

    ahead()
    for i in range(GRP):
        old_rows[:, i * BS : (i + 1) * BS] = dot(trans[...], raw_x[i, 0 : K * ITERS, :], HIGHEST)
    receive_raw(ITERS)
    for i in range(GRP):
        next_ref[:, i * BS : (i + 1) * BS] = dot(
            inverses[ITERS - 1], raw_x[i, K * ITERS :, :], HIGHEST
        )
    with scope("wait_last"):
        spread_last()
    _, coef, gram = receive_dots(ITERS)
    coef, gram = scaled(ITERS, coef, gram)
    next_ref[...] = next_ref[...] - dot(coef, old_rows[...], HIGHEST)
    normalise(ITERS, coef, gram)
    with scope("final"):
        record(ITERS, coef)
        next_ref[...] = dot(inverses[ITERS], next_ref[...], HIGHEST)
    await_send(last.at[pl.ds(0, CHIPS - 1)], last_send, last_recv)
    await_send(start_gram.at[0], pair_gram_send, pair_gram_recv)
    await_send(start_grams.at[pl.ds(0, CHIPS - 1)], gram_send, gram_recv)
    await_send(dots.at[ITERS, pl.ds(0, 7)], dots_send, dots_recv.at[0])


def write_out(*refs):
    inputs, outputs, sems = refs[:3], refs[3:6], refs[6]
    copies = [pltpu.make_async_copy(inputs[i], outputs[i], sems.at[i]) for i in (2, 0, 1)]
    for copy in copies:
        copy.start()
    for copy in copies:
        copy.wait()


def per_device(tiles, tile_rows, tile_cols, live_tiles, dual_shift, start_block):
    hbm = pl.BlockSpec(memory_space=pltpu.HBM)
    vmem = pl.BlockSpec(memory_space=pltpu.VMEM)
    in_hbm = functools.partial(pltpu.with_memory_space_constraint, memory_space=pltpu.HBM)
    dma = pltpu.SemaphoreType.DMA
    steps = ITERS + 1
    out = pl.pallas_call(
        kernel,
        out_shape=(
            pltpu.VMEM((ITERS, K, ITERS * K), F32),
            pltpu.VMEM((ITERS, K, K), F32),
            pltpu.VMEM((K, GRP * BS), F32),
        ),
        in_specs=[hbm] * 6,
        out_specs=(vmem, vmem, vmem),
        scratch_shapes=[
            pltpu.SMEM((1, 1, TILES), jnp.int32),
            pltpu.SMEM((1, 1, TILES), jnp.int32),
            pltpu.SMEM((1, 1), jnp.int32),
            pltpu.VMEM((1, GRP * BS), F32),
            pltpu.VMEM((K, K), F32),
            pltpu.VMEM((2, 8, 128), F32),
            pltpu.VMEM((CHIPS, 8, 128), F32),
            pltpu.VMEM((1, GRP * ROW), jnp.int32),
            pltpu.SMEM((1, GRP * ROW), jnp.int32),
            pltpu.VMEM((K, GRP * BS), F32),
            pltpu.VMEM((TILES, BS, BS), BF16),
            pltpu.VMEM((TILES, BS, BS), BF16),
            *[pltpu.VMEM((ROW, height(step), BS), BF16) for step in range(ITERS)],
            *[pltpu.VMEM((GRP, height(step), BS), BF16) for step in range(ITERS)],
            pltpu.VMEM((GRP, K * steps, BS), F32),
            pltpu.VMEM((K * ITERS, 2 * BS), F32),
            pltpu.VMEM((K * ITERS, BS), F32),
            pltpu.VMEM((K * ITERS, GRP * BS), F32),
            pltpu.VMEM((K * ITERS, K * ITERS), F32),
            pltpu.VMEM((TILES + 1, K, BS), F32),
            pltpu.VMEM((ITERS, CHIPS, K, BS), BF16),
            pltpu.VMEM((ITERS, CHIPS, K, BS), BF16),
            pltpu.VMEM((ITERS, CHIPS, K, BS), BF16),
            pltpu.VMEM((ITERS, CHIPS, K, BS), BF16),
            pltpu.VMEM((CHIPS, K, BS), F32),
            pltpu.VMEM((K, BS), F32),
            pltpu.VMEM((ITERS, GRP, K, BS), BF16),
            pltpu.VMEM((ITERS, GRP, K, BS), BF16),
            pltpu.VMEM((steps, 2 * GRP, K + 8, 128), F32),
            pltpu.VMEM((CHIPS, K + 8, 128), F32),
            dma((5,)),
            dma,
            dma,
            dma,
            dma,
            dma,
            dma,
            dma,
            dma,
            dma,
            dma((2, len(WAVES))),
            *[dma, dma((2,))] * 7,
        ],
        compiler_params=pltpu.CompilerParams(
            collective_id=0, has_side_effects=True, vmem_limit_bytes=48 * 1024 * 1024
        ),
        name="lanczos",
    )(
        in_hbm(tile_rows),
        in_hbm(tile_cols),
        live_tiles,
        *[
            in_hbm(a)
            for a in (
                tiles.reshape(TILES, BS, BS),
                start_block,
                dual_shift.reshape(1, GRP * BS),
            )
        ]
    )
    return pl.pallas_call(
        write_out,
        out_shape=tuple(jax.ShapeDtypeStruct(a.shape, a.dtype) for a in out),
        in_specs=[vmem] * 3,
        out_specs=(hbm, hbm, hbm),
        scratch_shapes=[dma((3,))],
        compiler_params=pltpu.CompilerParams(vmem_limit_bytes=1024 * 1024),
        name="write_out",
    )(*[pltpu.with_memory_space_constraint(a, pltpu.VMEM) for a in out])


def solution(mesh):
    in_specs = (
        P("grp", "row", None, None, None),
        P("grp", "row", None),
        P("grp", "row", None),
        P("grp", "row"),
        P("row"),
        P(None, "row"),
    )
    out_specs = (P(), P(), P(None, "row"))
    return jax.shard_map(
        per_device, mesh=mesh, in_specs=in_specs, out_specs=out_specs, check_vma=False
    )
```

```python
import contextlib
import functools

import jax
import jax.numpy as jnp
from jax import lax
from jax.experimental import pallas as pl
from jax.experimental.pallas import tpu as pltpu
from jax.sharding import PartitionSpec as P

MESH = pl.DeviceIdType.MESH
HIGHEST = lax.Precision.HIGHEST
F32 = jnp.float32
BF16 = jnp.bfloat16

ITERS = 4
K = 32
BS = 256
GRP = 4
ROW = 32
CHIPS = ROW // 2
SIDE = 4
TILES = 32
WAVES = (5, 5, 3, 2)
PARTS = 4
SHIFT = -1.0

FAR_FIRST = sorted(
    [(dz, dx) for dz in range(SIDE) for dx in range(SIDE) if (dz, dx) != (0, 0)],
    key=lambda d: -(min(d[0], SIDE - d[0]) + min(d[1], SIDE - d[1])),
)
SMALL_GROUP = [(dy, dc) for dy in (2, 1, 3, 0) for dc in (1, 0) if (dy, dc) != (0, 0)]


def height(step):
    return 2 * K if step == 0 else K


@contextlib.contextmanager
def phase(name):
    with jax.named_scope(name):
        yield
    if name in ("update", "cholesky", "dots", "direct", "pairs"):
        pl.delay(1)


def wave_of(m):
    return next(w for w in range(len(WAVES)) if m < sum(WAVES[: w + 1]))


def dots_height(step):
    return {1: K // 2, ITERS: K + 8}.get(step, K)


def dot(left, right, precision=None):
    return lax.dot_general(
        left, right, (((1,), (0,)), ((), ())), precision=precision, preferred_element_type=F32
    )


def t_dot(left, right, precision=None):
    return lax.dot_general(
        left, right, (((0,), (0,)), ((), ())), precision=precision, preferred_element_type=F32
    )


def dot_t(left, right, precision=None):
    return lax.dot_general(
        left, right, (((1,), (1,)), ((), ())), precision=precision, preferred_element_type=F32
    )


def cholesky(gram):
    row = lax.broadcasted_iota(jnp.int32, (K, K), 0)
    col = lax.broadcasted_iota(jnp.int32, (K, K), 1)
    left = gram
    right = jnp.where(row == col, 1.0, 0.0).astype(F32)
    for k in range(0, K - 2, 2):
        first = jnp.broadcast_to(left[:, k : k + 1], (K, K))
        second = jnp.broadcast_to(left[:, k + 1 : k + 2], (K, K))
        a = first[k : k + 1, :]
        b = second[k : k + 1, :]
        d = second[k + 1 : k + 2, :]
        inverse = 1.0 / (a * d - b * b)
        below = row > k + 1
        of_first = jnp.where(below, first * (d * inverse) - second * (b * inverse), 0.0)
        of_second = jnp.where(below, second * (a * inverse) - first * (b * inverse), 0.0)
        left_k, left_l = left[k : k + 1, :], left[k + 1 : k + 2, :]
        right_k, right_l = right[k : k + 1, :], right[k + 1 : k + 2, :]
        left = left - of_first * left_k - of_second * left_l
        right = right - of_first * right_k - of_second * right_l
    odd = (row & 1) == 1
    pivots = jnp.sum(jnp.where(row == col, left, 0.0), axis=1, keepdims=True)
    beside = jnp.sum(jnp.where(row + 1 == col, left, 0.0), axis=1, keepdims=True)
    factor = jnp.where(odd, pltpu.roll(jnp.broadcast_to(beside / pivots, (K, K)), 1, 0), 0.0)
    left = left - factor * pltpu.roll(left, 1, 0)
    right = right - factor * pltpu.roll(right, 1, 0)
    pivots = jnp.sum(jnp.where(row == col, left, 0.0), axis=1, keepdims=True)
    scale = 1.0 / jnp.sqrt(pivots)
    return jnp.where(col >= row, left * scale, 0.0), jnp.where(col <= row, right * scale, 0.0)


def kernel(
    rows_hbm,
    cols_hbm,
    live_hbm,
    tiles_hbm,
    start_hbm,
    dual_hbm,
    proj_ref,
    fact_ref,
    next_ref,
    rows_smem,
    cols_smem,
    live_smem,
    dual_ref,
    gram_ref,
    start_gram,
    start_grams,
    slot_vmem,
    slot_ref,
    start_ref,
    tiles,
    turned,
    cols_0,
    cols_1,
    cols_2,
    cols_3,
    rows_0,
    rows_1,
    rows_2,
    rows_3,
    raw_x,
    basis,
    in_blocks,
    old_rows,
    trans,
    products,
    pair_out,
    pair_in,
    back_out,
    back_in,
    own_back,
    own_direct,
    direct_out,
    direct_in,
    dots,
    last,
    load_sem,
    slot_sem,
    tile_sem,
    pair_gram_send,
    pair_gram_recv,
    gram_send,
    gram_recv,
    last_send,
    last_recv,
    cols_send,
    cols_recv,
    relay_send,
    relay_recv,
    rows_send,
    rows_recv,
    raw_send,
    raw_recv,
    dots_send,
    dots_recv,
    pair_send,
    pair_recv,
    back_send,
    back_recv,
    direct_send,
    direct_recv,
):
    cols_x = (cols_0, cols_1, cols_2, cols_3)
    rows_x = (rows_0, rows_1, rows_2, rows_3)
    g = lax.axis_index("grp")
    r = lax.axis_index("row")
    core = lax.rem(r, 2)
    chip = lax.div(r, 2)
    z = lax.div(chip, SIDE)
    x = lax.rem(chip, SIDE)
    partner = r + 1 - 2 * core

    def chip_at(dz, dx):
        return lax.rem(z + dz, SIDE) * SIDE + lax.rem(x + dx, SIDE)

    def chip_from(dz, dx):
        return lax.rem(z + SIDE - dz, SIDE) * SIDE + lax.rem(x + SIDE - dx, SIDE)

    def remote(src, dst, send, recv, group, owner):
        return pltpu.make_async_remote_copy(
            src_ref=src,
            dst_ref=dst,
            send_sem=send,
            recv_sem=recv,
            device_id=(group, owner),
            device_id_type=MESH,
        )

    def await_recv(ref, send, recv):
        remote(ref, ref, send, recv, g, partner).wait_recv()

    def await_send(ref, send, recv):
        remote(ref, ref, send, recv, g, partner).wait_send()

    barrier = pltpu.get_barrier_semaphore()
    for dz, dx in FAR_FIRST:
        pl.semaphore_signal(
            barrier, inc=1, device_id=(g, chip_at(dz, dx) * 2 + core), device_id_type=MESH
        )
    for dy, dc in SMALL_GROUP:
        pl.semaphore_signal(
            barrier,
            inc=1,
            device_id=(lax.rem(g + dy, GRP), partner if dc else r),
            device_id_type=MESH,
        )

    loads = [
        pltpu.make_async_copy(src, dst, load_sem.at[i])
        for i, (src, dst) in enumerate(
            [
                (rows_hbm, rows_smem),
                (cols_hbm, cols_smem),
                (live_hbm, live_smem),
                (start_hbm, start_ref),
                (dual_hbm, dual_ref),
            ]
        )
    ]
    for copy in loads:
        copy.start()
    load = pltpu.make_async_copy(tiles_hbm, tiles, tile_sem)
    load.start()

    trans[...] = jnp.zeros_like(trans)
    products[TILES] = jnp.zeros((K, BS), F32)
    proj_ref[...] = jnp.zeros_like(proj_ref)
    for copy in loads:
        copy.wait()

    lane = lax.broadcasted_iota(jnp.int32, (1, GRP * ROW), 1)
    slots = jnp.full((1, GRP * ROW), TILES, jnp.int32)
    for k in range(TILES):
        place = jnp.where(live_smem[0, 0] > k, rows_smem[0, 0, k] * ROW + cols_smem[0, 0, k], -1)
        slots = jnp.where(lane == place, k, slots)
    slot_vmem[...] = slots
    table = pltpu.make_async_copy(slot_vmem, slot_ref, slot_sem)
    table.start()

    for i in range(GRP):
        block = start_ref[:, i * BS : (i + 1) * BS]
        high = block.astype(BF16)
        rows_0[i, 0:K, :] = high
        rows_0[i, K : 2 * K, :] = (block - high.astype(F32)).astype(BF16)
        raw_x[i, 0:K, :] = block
    cols_0[r] = rows_0[g]
    gram = dot_t(start_ref[...], start_ref[...], HIGHEST)
    for i in range(4):
        start_gram[core, :, i * K : (i + 1) * K] = gram[8 * i : 8 * i + 8]
    dual = dual_ref[:, pl.ds(pl.multiple_of(g * BS, BS), BS)]

    def send_cols(step):
        here = cols_x[step].at[r]
        for m, (dz, dx) in enumerate(FAR_FIRST):
            remote(
                here, here, cols_send, cols_recv.at[step % 2, wave_of(m)], g, chip_at(dz, dx) * 2 + core
            ).start()
        remote(here, here, relay_send, relay_recv.at[step % 2], g, partner).start()

    def receive_cols(step):
        first = 0
        for wave, count in enumerate(WAVES):
            await_recv(
                cols_x[step].at[pl.ds(0, count)], cols_send, cols_recv.at[step % 2, wave]
            )
            for m in range(first, first + count):
                there = cols_x[step].at[chip_from(*FAR_FIRST[m]) * 2 + core]
                remote(there, there, relay_send, relay_recv.at[step % 2], g, partner).start()
            first += count

    def sent(step):
        await_send(cols_x[step].at[pl.ds(0, CHIPS - 1)], cols_send, cols_recv.at[0, 0])
        await_send(cols_x[step].at[pl.ds(0, CHIPS)], relay_send, relay_recv.at[0])
        await_send(pair_out.at[step], pair_send, pair_recv.at[0])
        await_send(back_in.at[step, pl.ds(0, CHIPS - 1)], back_send, back_recv.at[0])
        await_send(direct_in.at[step, pl.ds(0, 3)], direct_send, direct_recv.at[0])
        if step > 0:
            await_send(rows_x[step].at[pl.ds(0, 3)], rows_send, rows_recv.at[0])
            await_send(dots.at[step, pl.ds(0, 7), pl.ds(0, dots_height(step))], dots_send, dots_recv.at[0])

    def send_raw(step):
        if step > 1:
            receive_raw(step - 1)
        mine = raw_x.at[g, pl.ds(K * step, K), :]
        for dy in (2, 1, 3):
            remote(
                mine, mine, raw_send, raw_recv.at[step % 2], lax.rem(g + dy, GRP), r
            ).start()

    def receive_raw(step):
        others = raw_x.at[pl.ds(0, 3), pl.ds(K * step, K), :]
        await_recv(others, raw_send, raw_recv.at[step % 2])
        await_send(others, raw_send, raw_recv.at[step % 2])

    def products_of(load_left, rows, matrices):
        def body(k, carry):
            product = dot(load_left(k), matrices[k])
            if rows == 2 * K:
                product = product[:K] + product[K:]
            products[k] = product
            return carry

        lax.fori_loop(0, TILES, body, 0, unroll=True)

    def back_sum(owner):
        total = products[slot_ref[0, owner]]
        for i in range(1, GRP):
            total = total + products[slot_ref[0, i * ROW + owner]]
        return total

    def send_pairs(step):
        for part in range(PARTS):

            def other(m, carry):
                pair_out[step, m] = back_sum(m * 2 + 1 - core).astype(BF16)
                return carry

            size = CHIPS // PARTS
            lax.fori_loop(part * size, part * size + size, other, 0, unroll=2)
            here = pl.ds(part * size, size)
            remote(
                pair_out.at[step, here],
                pair_in.at[step, here],
                pair_send,
                pair_recv.at[step % 2],
                g,
                partner,
            ).start()

    def own_sums(step):
        def mine(m, carry):
            own_back[m] = back_sum(m * 2 + core)
            return carry

        lax.fori_loop(0, CHIPS, mine, 0, unroll=2)

    def send_back(step):
        with phase("wait_pair"):
            await_recv(pair_in.at[step], pair_send, pair_recv.at[step % 2])
        for dz, dx in FAR_FIRST:
            there = chip_at(dz, dx)
            back_out[step, there] = (
                own_back[there] + pair_in[step, there].astype(F32)
            ).astype(BF16)
        for dz, dx in FAR_FIRST:
            there = chip_at(dz, dx)
            remote(
                back_out.at[step, there],
                back_in.at[step, chip],
                back_send,
                back_recv.at[step % 2],
                g,
                there * 2 + core,
            ).start()

    def send_direct(step):
        for dy in (2, 1, 3, 0):
            group = lax.rem(g + dy, GRP)

            def add(j, total, group=group):
                return total + products[slot_ref[0, group * ROW + j]]

            total = lax.fori_loop(0, ROW, add, jnp.zeros((K, BS), F32), unroll=8)
            if dy == 0:
                own_direct[...] = total
                continue
            direct_out[step, group] = total.astype(BF16)
            remote(
                direct_out.at[step, group],
                direct_in.at[step, g],
                direct_send,
                direct_recv.at[step % 2],
                group,
                r,
            ).start()

    def send_start_gram():
        await_recv(start_gram.at[0], pair_gram_send, pair_gram_recv)
        start_grams[chip] = start_gram[0] + start_gram[1]
        mine = start_grams.at[chip]
        for dz, dx in FAR_FIRST:
            remote(mine, mine, gram_send, gram_recv, g, chip_at(dz, dx) * 2 + core).start()

    def receive_start_gram():
        await_recv(start_grams.at[pl.ds(0, CHIPS - 1)], gram_send, gram_recv)
        total = start_grams[0]
        for i in range(1, CHIPS):
            total = total + start_grams[i]
        return jnp.concatenate([total[:, i * K : (i + 1) * K] for i in range(4)], axis=0)

    def send_dots(step):
        width = K * step + K

        totals = [jnp.zeros((K, width), F32) for _ in range(4)]
        for p in range(CHIPS):
            owner = p * 2 + core
            so_far = jnp.concatenate([cols_x[s][owner, 0:K] for s in range(step + 1)], axis=0)
            totals[p % 4] = totals[p % 4] + dot_t(cols_x[step][owner], so_far)
        total = (totals[0] + totals[1]) + (totals[2] + totals[3])
        here = g * 2 + core
        if step == 1:
            dots[1, here, 0 : K // 2, 0:width] = total[: K // 2]
            dots[1, here, 0 : K // 2, width:] = total[K // 2 :]
        else:
            dots[step, here, 0:K, 0:width] = total
        spread_dots(step)

    def spread_dots(step):
        here = g * 2 + core
        mine = dots.at[step, here, pl.ds(0, dots_height(step))]
        for dy, dc in SMALL_GROUP:
            remote(
                mine,
                mine,
                dots_send,
                dots_recv.at[step % 2],
                lax.rem(g + dy, GRP),
                partner if dc else r,
            ).start()

    def send_last():
        block = raw_x[g, K * ITERS :, :]
        total = dot_t(block, raw_x[g], HIGHEST)
        last[chip, 0:K, :] = total[:, 0 : K * ITERS]
        gram = total[:, K * ITERS :]
        for i in range(4):
            last[chip, K:, i * K : (i + 1) * K] = gram[8 * i : 8 * i + 8]
        mine = last.at[chip]
        for dz, dx in FAR_FIRST:
            remote(mine, mine, last_send, last_recv, g, chip_at(dz, dx) * 2 + core).start()

    def spread_last():
        await_recv(last.at[pl.ds(0, CHIPS - 1)], last_send, last_recv)
        total = last[0]
        for i in range(1, CHIPS):
            total = total + last[i]
        dots[ITERS, g * 2 + core] = total
        spread_dots(ITERS)

    def receive_dots(step):
        with phase("wait_dots"):
            await_recv(
                dots.at[step, pl.ds(0, 7), pl.ds(0, dots_height(step))],
                dots_send,
                dots_recv.at[step % 2],
            )
        total = dots[step, 0, 0 : dots_height(step)]
        for i in range(1, 2 * GRP):
            total = total + dots[step, i, 0 : dots_height(step)]
        if step == 1:
            total = jnp.concatenate([total[:, : 2 * K], total[:, 2 * K :]], axis=0)
        if step < ITERS:
            gram = total[:, K * step : K + K * step]
        else:
            gram = jnp.concatenate([total[K:, i * K : (i + 1) * K] for i in range(4)], axis=0)
        products_before = total[0:K, : K * step]
        coef = dot_t(products_before, trans[0 : K * step, 0 : K * step], HIGHEST)
        return products_before, coef, gram - dot_t(coef, coef, HIGHEST)

    def settle(gram):
        gram_ref[...] = gram
        return gram_ref[...]

    def scaled(step, coef, gram):
        if step > 1:
            coef = dot(inverses[step - 1], coef, HIGHEST)
            gram = dot_t(dot(inverses[step - 1], gram, HIGHEST), inverses[step - 1], HIGHEST)
        return coef, settle(gram)

    def normalise(step, coef, gram):
        with phase("cholesky"):
            upper, inverse = cholesky(gram)
        if step > 0:
            fact_ref[step - 1] = upper.T
        if step < ITERS:
            own = inverse if step < 2 else dot(inverse, inverses[step - 1], HIGHEST)
            trans[K * step : K + K * step, K * step : K + K * step] = own
            if step > 0:
                trans[K * step : K + K * step, 0 : K * step] = -dot(
                    inverse,
                    dot(coef, trans[0 : K * step, 0 : K * step], HIGHEST),
                    HIGHEST,
                )
        uppers[step] = upper
        inverses[step] = inverse

    def record(step, coef):
        row = lax.broadcasted_iota(jnp.int32, (K, K), 0)
        col = lax.broadcasted_iota(jnp.int32, (K, K), 1)
        at = K * (step - 1)
        if step > 1:
            if step > 2:
                proj_ref[step - 1, :, 0 : at - K] = coef[:, : at - K]
            proj_ref[step - 1, :, at - K : at] = coef[:, at - K : at] + uppers[step - 1]
        proj_ref[step - 1, :, at : at + K] = coef[:, at:] + jnp.where(row == col, SHIFT, 0.0)

    uppers = {}
    inverses = {}
    scope = phase
    ahead = None
    for step in range(ITERS):
        size = height(step)
        if ahead is not None:
            newest = ahead()
        if step == 0:
            with scope("enter"):
                pl.semaphore_wait(barrier, len(FAR_FIRST) + len(SMALL_GROUP))
            mine = start_gram.at[core]
            remote(mine, mine, pair_gram_send, pair_gram_recv, g, partner).start()
            send_cols(0)
            with scope("load"):
                load.wait()
                table.wait()
            with scope("back"):
                products_of(lambda k: rows_0[rows_smem[0, 0, k]], size, tiles)
        else:
            with scope("wait_rows"):
                await_recv(rows_x[step].at[pl.ds(0, 3)], rows_send, rows_recv.at[step % 2])
            send_raw(step)
            with scope("back"):
                products_of(lambda k, step=step: rows_x[step][rows_smem[0, 0, k]], size, tiles)
        with scope("pairs"):
            send_pairs(step)
        with scope("own_sums"):
            own_sums(step)
            if step == 0:
                send_start_gram()
        if step == 0:
            with scope("turn"):

                def turn(k, carry):
                    turned[k] = tiles[k].T
                    return carry

                lax.fori_loop(0, TILES, turn, 0, unroll=2)

        @pl.when(core == 0)
        def _(step=step):
            send_back(step)

        with scope("wait_cols"):
            receive_cols(step)
        if step > 0:
            with scope("dots"):
                send_dots(step)

        @pl.when(core == 1)
        def _(step=step):
            send_back(step)

        with scope("wait_relay"):
            await_recv(cols_x[step].at[pl.ds(0, CHIPS)], relay_send, relay_recv.at[step % 2])
        with scope("forward"):
            products_of(lambda k, step=step: cols_x[step][cols_smem[0, 0, k]], size, turned)
        with scope("direct"):
            send_direct(step)

        if step == 0:
            with scope("wait_dots"):
                coef, gram = None, receive_start_gram()
            normalise(0, None, gram)
            first = dot(inverses[0], raw_x[g, 0:K, :], HIGHEST)
            known = first * (-SHIFT)
            basis[0:K, 0:BS] = first
        else:
            before, coef, gram = receive_dots(step)
            with scope("known"):
                known = raw_x[g, K * step : K * step + K, :] * (-SHIFT)
                known = known - dot(before, in_blocks[0 : K * step, :], HIGHEST)
                known = known - dot(gram, newest, HIGHEST)

        sent(step)
        with scope("wait_direct"):
            await_recv(
                direct_in.at[step, pl.ds(0, 3)], direct_send, direct_recv.at[step % 2]
            )
        with scope("wait_back"):
            await_recv(
                back_in.at[step, pl.ds(0, CHIPS - 1)], back_send, back_recv.at[step % 2]
            )
        with scope("update"):
            total = own_direct[...]
            for dy in (1, 2, 3):
                total = total + direct_in[step, lax.rem(g + dy, GRP)].astype(F32)
            total = total + own_back[chip] + pair_in[step, chip].astype(F32)
            for dz, dx in FAR_FIRST:
                total = total + back_in[step, chip_at(dz, dx)].astype(F32)
            image = 0.5 * total - raw_x[g, K * step : K * step + K, :] * dual
            if step == 0:
                image = dot(inverses[0], image, HIGHEST)
                basis[0:K, BS:] = image
                following = image + known
            elif step == 1:
                following = image + known
            else:
                following = dot(inverses[step - 1], image + known, HIGHEST)
            rounded = following.astype(BF16)
            after = step + 1
            raw_x[g, K * after : K * after + K, :] = following
            if after < ITERS:
                cols_x[after][r] = rounded
                rows_x[after][g] = rounded
                mine = rows_x[after].at[g]
                for dy in (2, 1, 3):
                    remote(
                        mine,
                        mine,
                        rows_send,
                        rows_recv.at[after % 2],
                        lax.rem(g + dy, GRP),
                        r,
                    ).start()
                send_cols(after)
            else:
                send_last()
                send_raw(after)

        def ahead(step=step, coef=coef, gram=gram, image=image):
            at = K * step
            if step > 0:
                coef, gram = scaled(step, coef, gram)
                normalise(step, coef, gram)
                both = jnp.concatenate([raw_x[g, at : at + K, :], image], axis=1)
                if step > 1:
                    both = dot(inverses[step - 1], both, HIGHEST)
                both = both - dot(coef, basis[0:at, :], HIGHEST)
                basis[at : at + K, :] = dot(inverses[step], both, HIGHEST)
                record(step, coef)
            if step == ITERS - 1:
                return None
            size = at + K
            in_blocks[0:size, :] = t_dot(
                trans[0:size, 0:size],
                basis[0:size, BS:] - SHIFT * basis[0:size, 0:BS],
                HIGHEST,
            )
            last = basis[at : at + K, 0:BS]
            return last if step == 0 else t_dot(inverses[step], last, HIGHEST)

    ahead()
    for i in range(GRP):
        old_rows[:, i * BS : (i + 1) * BS] = dot(trans[...], raw_x[i, 0 : K * ITERS, :], HIGHEST)
    receive_raw(ITERS)
    with scope("wait_last"):
        spread_last()
    _, coef, gram = receive_dots(ITERS)
    gram = settle(gram)
    for i in range(GRP):
        here = slice(i * BS, (i + 1) * BS)
        next_ref[:, here] = raw_x[i, K * ITERS :, :] - dot(coef, old_rows[:, here], HIGHEST)
    with scope("cholesky"):
        upper, inverse = cholesky(gram)
    with scope("final"):
        next_ref[...] = dot(inverse, next_ref[...], HIGHEST)
        fact_ref[ITERS - 1] = dot_t(inverses[ITERS - 1], upper, HIGHEST)
        record(ITERS, dot(inverses[ITERS - 1], coef, HIGHEST))

    await_send(last.at[pl.ds(0, CHIPS - 1)], last_send, last_recv)
    await_send(start_gram.at[0], pair_gram_send, pair_gram_recv)
    await_send(start_grams.at[pl.ds(0, CHIPS - 1)], gram_send, gram_recv)
    await_send(dots.at[ITERS, pl.ds(0, 7)], dots_send, dots_recv.at[0])


def write_out(*refs):
    inputs, outputs, sems = refs[:3], refs[3:6], refs[6]
    copies = [pltpu.make_async_copy(inputs[i], outputs[i], sems.at[i]) for i in (2, 0, 1)]
    for copy in copies:
        copy.start()
    for copy in copies:
        copy.wait()


def per_device(tiles, tile_rows, tile_cols, live_tiles, dual_shift, start_block):
    hbm = pl.BlockSpec(memory_space=pltpu.HBM)
    vmem = pl.BlockSpec(memory_space=pltpu.VMEM)
    in_hbm = functools.partial(pltpu.with_memory_space_constraint, memory_space=pltpu.HBM)
    dma = pltpu.SemaphoreType.DMA
    steps = ITERS + 1
    out = pl.pallas_call(
        kernel,
        out_shape=(
            pltpu.VMEM((ITERS, K, ITERS * K), F32),
            pltpu.VMEM((ITERS, K, K), F32),
            pltpu.VMEM((K, GRP * BS), F32),
        ),
        in_specs=[hbm] * 6,
        out_specs=(vmem, vmem, vmem),
        scratch_shapes=[
            pltpu.SMEM((1, 1, TILES), jnp.int32),
            pltpu.SMEM((1, 1, TILES), jnp.int32),
            pltpu.SMEM((1, 1), jnp.int32),
            pltpu.VMEM((1, GRP * BS), F32),
            pltpu.VMEM((K, K), F32),
            pltpu.VMEM((2, 8, 128), F32),
            pltpu.VMEM((CHIPS, 8, 128), F32),
            pltpu.VMEM((1, GRP * ROW), jnp.int32),
            pltpu.SMEM((1, GRP * ROW), jnp.int32),
            pltpu.VMEM((K, GRP * BS), F32),
            pltpu.VMEM((TILES, BS, BS), BF16),
            pltpu.VMEM((TILES, BS, BS), BF16),
            *[pltpu.VMEM((ROW, height(step), BS), BF16) for step in range(ITERS)],
            *[pltpu.VMEM((GRP, height(step), BS), BF16) for step in range(ITERS)],
            pltpu.VMEM((GRP, K * steps, BS), F32),
            pltpu.VMEM((K * ITERS, 2 * BS), F32),
            pltpu.VMEM((K * ITERS, BS), F32),
            pltpu.VMEM((K * ITERS, GRP * BS), F32),
            pltpu.VMEM((K * ITERS, K * ITERS), F32),
            pltpu.VMEM((TILES + 1, K, BS), F32),
            pltpu.VMEM((ITERS, CHIPS, K, BS), BF16),
            pltpu.VMEM((ITERS, CHIPS, K, BS), BF16),
            pltpu.VMEM((ITERS, CHIPS, K, BS), BF16),
            pltpu.VMEM((ITERS, CHIPS, K, BS), BF16),
            pltpu.VMEM((CHIPS, K, BS), F32),
            pltpu.VMEM((K, BS), F32),
            pltpu.VMEM((ITERS, GRP, K, BS), BF16),
            pltpu.VMEM((ITERS, GRP, K, BS), BF16),
            pltpu.VMEM((steps, 2 * GRP, K + 8, 128), F32),
            pltpu.VMEM((CHIPS, K + 8, 128), F32),
            dma((5,)),
            dma,
            dma,
            dma,
            dma,
            dma,
            dma,
            dma,
            dma,
            dma,
            dma((2, len(WAVES))),
            *[dma, dma((2,))] * 7,
        ],
        compiler_params=pltpu.CompilerParams(
            collective_id=0, has_side_effects=True, vmem_limit_bytes=48 * 1024 * 1024
        ),
        name="lanczos",
    )(
        in_hbm(tile_rows),
        in_hbm(tile_cols),
        live_tiles,
        *[
            in_hbm(a)
            for a in (
                tiles.reshape(TILES, BS, BS),
                start_block,
                dual_shift.reshape(1, GRP * BS),
            )
        ]
    )
    return pl.pallas_call(
        write_out,
        out_shape=tuple(jax.ShapeDtypeStruct(a.shape, a.dtype) for a in out),
        in_specs=[vmem] * 3,
        out_specs=(hbm, hbm, hbm),
        scratch_shapes=[dma((3,))],
        compiler_params=pltpu.CompilerParams(vmem_limit_bytes=1024 * 1024),
        name="write_out",
    )(*[pltpu.with_memory_space_constraint(a, pltpu.VMEM) for a in out])


def solution(mesh):
    in_specs = (
        P("grp", "row", None, None, None),
        P("grp", "row", None),
        P("grp", "row", None),
        P("grp", "row"),
        P("row"),
        P(None, "row"),
    )
    out_specs = (P(), P(), P(None, "row"))
    return jax.shard_map(
        per_device, mesh=mesh, in_specs=in_specs, out_specs=out_specs, check_vma=False
    )
```

```python
import contextlib
import functools

import jax
import jax.numpy as jnp
from jax import lax
from jax.experimental import pallas as pl
from jax.experimental.pallas import tpu as pltpu
from jax.sharding import PartitionSpec as P

MESH = pl.DeviceIdType.MESH
HIGHEST = lax.Precision.HIGHEST
F32 = jnp.float32
BF16 = jnp.bfloat16

ITERS = 4
K = 32
BS = 256
GRP = 4
ROW = 32
CHIPS = ROW // 2
SIDE = 4
TILES = 32
WAVES = (4, 3, 2, 2, 2, 1, 1)
PARTS = 4
SHIFT = -1.0

FAR_FIRST = sorted(
    [(dz, dx) for dz in range(SIDE) for dx in range(SIDE) if (dz, dx) != (0, 0)],
    key=lambda d: -(min(d[0], SIDE - d[0]) + min(d[1], SIDE - d[1])),
)
SMALL_GROUP = [(dy, dc) for dy in (2, 1, 3, 0) for dc in (1, 0) if (dy, dc) != (0, 0)]


def height(step):
    return 2 * K if step == 0 else K


@contextlib.contextmanager
def phase(name):
    with jax.named_scope(name):
        yield
    if name in ("update", "cholesky", "dots", "direct", "pairs"):
        pl.delay(1)


def wave_of(m):
    return next(w for w in range(len(WAVES)) if m < sum(WAVES[: w + 1]))


def dots_height(step):
    return {1: K // 2, ITERS: K + 8}.get(step, K)


def dot(left, right, precision=None):
    return lax.dot_general(
        left, right, (((1,), (0,)), ((), ())), precision=precision, preferred_element_type=F32
    )


def t_dot(left, right, precision=None):
    return lax.dot_general(
        left, right, (((0,), (0,)), ((), ())), precision=precision, preferred_element_type=F32
    )


def dot_t(left, right, precision=None):
    return lax.dot_general(
        left, right, (((1,), (1,)), ((), ())), precision=precision, preferred_element_type=F32
    )


def cholesky(gram):
    row = lax.broadcasted_iota(jnp.int32, (K, K), 0)
    col = lax.broadcasted_iota(jnp.int32, (K, K), 1)
    left = gram
    right = jnp.where(row == col, 1.0, 0.0).astype(F32)
    for k in range(0, K - 2, 2):
        first = jnp.broadcast_to(left[:, k : k + 1], (K, K))
        second = jnp.broadcast_to(left[:, k + 1 : k + 2], (K, K))
        a = first[k : k + 1, :]
        b = second[k : k + 1, :]
        d = second[k + 1 : k + 2, :]
        inverse = 1.0 / (a * d - b * b)
        below = row > k + 1
        of_first = jnp.where(below, first * (d * inverse) - second * (b * inverse), 0.0)
        of_second = jnp.where(below, second * (a * inverse) - first * (b * inverse), 0.0)
        left_k, left_l = left[k : k + 1, :], left[k + 1 : k + 2, :]
        right_k, right_l = right[k : k + 1, :], right[k + 1 : k + 2, :]
        left = left - of_first * left_k - of_second * left_l
        right = right - of_first * right_k - of_second * right_l
    odd = (row & 1) == 1
    pivots = jnp.sum(jnp.where(row == col, left, 0.0), axis=1, keepdims=True)
    beside = jnp.sum(jnp.where(row + 1 == col, left, 0.0), axis=1, keepdims=True)
    factor = jnp.where(odd, pltpu.roll(jnp.broadcast_to(beside / pivots, (K, K)), 1, 0), 0.0)
    left = left - factor * pltpu.roll(left, 1, 0)
    right = right - factor * pltpu.roll(right, 1, 0)
    pivots = jnp.sum(jnp.where(row == col, left, 0.0), axis=1, keepdims=True)
    scale = 1.0 / jnp.sqrt(pivots)
    return jnp.where(col >= row, left * scale, 0.0), jnp.where(col <= row, right * scale, 0.0)


def kernel(
    rows_hbm,
    cols_hbm,
    live_hbm,
    tiles_hbm,
    start_hbm,
    dual_hbm,
    proj_ref,
    fact_ref,
    next_ref,
    rows_smem,
    cols_smem,
    live_smem,
    dual_ref,
    gram_ref,
    start_gram,
    start_grams,
    slot_vmem,
    slot_ref,
    start_ref,
    tiles,
    turned,
    cols_0,
    cols_1,
    cols_2,
    cols_3,
    rows_0,
    rows_1,
    rows_2,
    rows_3,
    raw_x,
    basis,
    in_blocks,
    old_rows,
    trans,
    products,
    pair_out,
    pair_in,
    back_out,
    back_in,
    own_back,
    own_direct,
    direct_out,
    direct_in,
    dots,
    last,
    load_sem,
    slot_sem,
    tile_sem,
    pair_gram_send,
    pair_gram_recv,
    gram_send,
    gram_recv,
    last_send,
    last_recv,
    cols_send,
    cols_recv,
    relay_send,
    relay_recv,
    rows_send,
    rows_recv,
    raw_send,
    raw_recv,
    dots_send,
    dots_recv,
    pair_send,
    pair_recv,
    back_send,
    back_recv,
    direct_send,
    direct_recv,
):
    cols_x = (cols_0, cols_1, cols_2, cols_3)
    rows_x = (rows_0, rows_1, rows_2, rows_3)
    g = lax.axis_index("grp")
    r = lax.axis_index("row")
    core = lax.rem(r, 2)
    chip = lax.div(r, 2)
    z = lax.div(chip, SIDE)
    x = lax.rem(chip, SIDE)
    partner = r + 1 - 2 * core

    def chip_at(dz, dx):
        return lax.rem(z + dz, SIDE) * SIDE + lax.rem(x + dx, SIDE)

    def chip_from(dz, dx):
        return lax.rem(z + SIDE - dz, SIDE) * SIDE + lax.rem(x + SIDE - dx, SIDE)

    def remote(src, dst, send, recv, group, owner):
        return pltpu.make_async_remote_copy(
            src_ref=src,
            dst_ref=dst,
            send_sem=send,
            recv_sem=recv,
            device_id=(group, owner),
            device_id_type=MESH,
        )

    def await_recv(ref, send, recv):
        remote(ref, ref, send, recv, g, partner).wait_recv()

    def await_send(ref, send, recv):
        remote(ref, ref, send, recv, g, partner).wait_send()

    barrier = pltpu.get_barrier_semaphore()
    for dz, dx in FAR_FIRST:
        pl.semaphore_signal(
            barrier, inc=1, device_id=(g, chip_at(dz, dx) * 2 + core), device_id_type=MESH
        )
    for dy, dc in SMALL_GROUP:
        pl.semaphore_signal(
            barrier,
            inc=1,
            device_id=(lax.rem(g + dy, GRP), partner if dc else r),
            device_id_type=MESH,
        )

    loads = [
        pltpu.make_async_copy(src, dst, load_sem.at[i])
        for i, (src, dst) in enumerate(
            [
                (rows_hbm, rows_smem),
                (cols_hbm, cols_smem),
                (live_hbm, live_smem),
                (start_hbm, start_ref),
                (dual_hbm, dual_ref),
            ]
        )
    ]
    for copy in loads:
        copy.start()
    load = pltpu.make_async_copy(tiles_hbm, tiles, tile_sem)
    load.start()

    trans[...] = jnp.zeros_like(trans)
    products[TILES] = jnp.zeros((K, BS), F32)
    proj_ref[...] = jnp.zeros_like(proj_ref)
    for copy in loads:
        copy.wait()

    lane = lax.broadcasted_iota(jnp.int32, (1, GRP * ROW), 1)
    slots = jnp.full((1, GRP * ROW), TILES, jnp.int32)
    for k in range(TILES):
        place = jnp.where(live_smem[0, 0] > k, rows_smem[0, 0, k] * ROW + cols_smem[0, 0, k], -1)
        slots = jnp.where(lane == place, k, slots)
    slot_vmem[...] = slots
    table = pltpu.make_async_copy(slot_vmem, slot_ref, slot_sem)
    table.start()

    for i in range(GRP):
        block = start_ref[:, i * BS : (i + 1) * BS]
        high = block.astype(BF16)
        rows_0[i, 0:K, :] = high
        rows_0[i, K : 2 * K, :] = (block - high.astype(F32)).astype(BF16)
        raw_x[i, 0:K, :] = block
    cols_0[r] = rows_0[g]
    gram = dot_t(start_ref[...], start_ref[...], HIGHEST)
    for i in range(4):
        start_gram[core, :, i * K : (i + 1) * K] = gram[8 * i : 8 * i + 8]
    dual = dual_ref[:, pl.ds(pl.multiple_of(g * BS, BS), BS)]

    def send_cols(step):
        here = cols_x[step].at[r]
        for m, (dz, dx) in enumerate(FAR_FIRST):
            remote(
                here, here, cols_send, cols_recv.at[step % 2, wave_of(m)], g, chip_at(dz, dx) * 2 + core
            ).start()
        remote(here, here, relay_send, relay_recv.at[step % 2], g, partner).start()

    def receive_cols(step):
        first = 0
        for wave, count in enumerate(WAVES):
            await_recv(
                cols_x[step].at[pl.ds(0, count)], cols_send, cols_recv.at[step % 2, wave]
            )
            for m in range(first, first + count):
                there = cols_x[step].at[chip_from(*FAR_FIRST[m]) * 2 + core]
                remote(there, there, relay_send, relay_recv.at[step % 2], g, partner).start()
            first += count

    def sent(step):
        await_send(cols_x[step].at[pl.ds(0, CHIPS - 1)], cols_send, cols_recv.at[0, 0])
        await_send(cols_x[step].at[pl.ds(0, CHIPS)], relay_send, relay_recv.at[0])
        await_send(pair_out.at[step], pair_send, pair_recv.at[0])
        await_send(back_in.at[step, pl.ds(0, CHIPS - 1)], back_send, back_recv.at[0])
        await_send(direct_in.at[step, pl.ds(0, 3)], direct_send, direct_recv.at[0])
        if step > 0:
            await_send(rows_x[step].at[pl.ds(0, 3)], rows_send, rows_recv.at[0])
            await_send(dots.at[step, pl.ds(0, 7), pl.ds(0, dots_height(step))], dots_send, dots_recv.at[0])

    def send_raw(step):
        if step > 1:
            receive_raw(step - 1)
        mine = raw_x.at[g, pl.ds(K * step, K), :]
        for dy in (2, 1, 3):
            remote(
                mine, mine, raw_send, raw_recv.at[step % 2], lax.rem(g + dy, GRP), r
            ).start()

    def receive_raw(step):
        others = raw_x.at[pl.ds(0, 3), pl.ds(K * step, K), :]
        await_recv(others, raw_send, raw_recv.at[step % 2])
        await_send(others, raw_send, raw_recv.at[step % 2])

    def products_of(load_left, rows, matrices):
        def body(k, carry):
            product = dot(load_left(k), matrices[k])
            if rows == 2 * K:
                product = product[:K] + product[K:]
            products[k] = product
            return carry

        lax.fori_loop(0, TILES, body, 0, unroll=True)

    def back_sum(owner):
        total = products[slot_ref[0, owner]]
        for i in range(1, GRP):
            total = total + products[slot_ref[0, i * ROW + owner]]
        return total

    def send_pairs(step):
        for part in range(PARTS):

            def other(m, carry):
                pair_out[step, m] = back_sum(m * 2 + 1 - core).astype(BF16)
                return carry

            size = CHIPS // PARTS
            lax.fori_loop(part * size, part * size + size, other, 0, unroll=2)
            here = pl.ds(part * size, size)
            remote(
                pair_out.at[step, here],
                pair_in.at[step, here],
                pair_send,
                pair_recv.at[step % 2],
                g,
                partner,
            ).start()

    def own_sums(step):
        def mine(m, carry):
            own_back[m] = back_sum(m * 2 + core)
            return carry

        lax.fori_loop(0, CHIPS, mine, 0, unroll=2)

    def send_back(step):
        with phase("wait_pair"):
            await_recv(pair_in.at[step], pair_send, pair_recv.at[step % 2])
        for dz, dx in FAR_FIRST:
            there = chip_at(dz, dx)
            back_out[step, there] = (
                own_back[there] + pair_in[step, there].astype(F32)
            ).astype(BF16)
        for dz, dx in FAR_FIRST:
            there = chip_at(dz, dx)
            remote(
                back_out.at[step, there],
                back_in.at[step, chip],
                back_send,
                back_recv.at[step % 2],
                g,
                there * 2 + core,
            ).start()

    def send_direct(step):
        for dy in (2, 1, 3, 0):
            group = lax.rem(g + dy, GRP)

            def add(j, total, group=group):
                return total + products[slot_ref[0, group * ROW + j]]

            total = lax.fori_loop(0, ROW, add, jnp.zeros((K, BS), F32), unroll=8)
            if dy == 0:
                own_direct[...] = total
                continue
            direct_out[step, group] = total.astype(BF16)
            remote(
                direct_out.at[step, group],
                direct_in.at[step, g],
                direct_send,
                direct_recv.at[step % 2],
                group,
                r,
            ).start()

    def send_start_gram():
        await_recv(start_gram.at[0], pair_gram_send, pair_gram_recv)
        start_grams[chip] = start_gram[0] + start_gram[1]
        mine = start_grams.at[chip]
        for dz, dx in FAR_FIRST:
            remote(mine, mine, gram_send, gram_recv, g, chip_at(dz, dx) * 2 + core).start()

    def receive_start_gram():
        await_recv(start_grams.at[pl.ds(0, CHIPS - 1)], gram_send, gram_recv)
        total = start_grams[0]
        for i in range(1, CHIPS):
            total = total + start_grams[i]
        return jnp.concatenate([total[:, i * K : (i + 1) * K] for i in range(4)], axis=0)

    def send_dots(step):
        width = K * step + K

        totals = [jnp.zeros((K, width), F32) for _ in range(4)]
        for p in range(CHIPS):
            owner = p * 2 + core
            so_far = jnp.concatenate([cols_x[s][owner, 0:K] for s in range(step + 1)], axis=0)
            totals[p % 4] = totals[p % 4] + dot_t(cols_x[step][owner], so_far)
        total = (totals[0] + totals[1]) + (totals[2] + totals[3])
        here = g * 2 + core
        if step == 1:
            dots[1, here, 0 : K // 2, 0:width] = total[: K // 2]
            dots[1, here, 0 : K // 2, width:] = total[K // 2 :]
        else:
            dots[step, here, 0:K, 0:width] = total
        spread_dots(step)

    def spread_dots(step):
        here = g * 2 + core
        mine = dots.at[step, here, pl.ds(0, dots_height(step))]
        for dy, dc in SMALL_GROUP:
            remote(
                mine,
                mine,
                dots_send,
                dots_recv.at[step % 2],
                lax.rem(g + dy, GRP),
                partner if dc else r,
            ).start()

    def send_last():
        block = raw_x[g, K * ITERS :, :]
        total = dot_t(block, raw_x[g], HIGHEST)
        last[chip, 0:K, :] = total[:, 0 : K * ITERS]
        gram = total[:, K * ITERS :]
        for i in range(4):
            last[chip, K:, i * K : (i + 1) * K] = gram[8 * i : 8 * i + 8]
        mine = last.at[chip]
        for dz, dx in FAR_FIRST:
            remote(mine, mine, last_send, last_recv, g, chip_at(dz, dx) * 2 + core).start()

    def spread_last():
        await_recv(last.at[pl.ds(0, CHIPS - 1)], last_send, last_recv)
        total = last[0]
        for i in range(1, CHIPS):
            total = total + last[i]
        dots[ITERS, g * 2 + core] = total
        spread_dots(ITERS)

    def receive_dots(step):
        with phase("wait_dots"):
            await_recv(
                dots.at[step, pl.ds(0, 7), pl.ds(0, dots_height(step))],
                dots_send,
                dots_recv.at[step % 2],
            )
        total = dots[step, 0, 0 : dots_height(step)]
        for i in range(1, 2 * GRP):
            total = total + dots[step, i, 0 : dots_height(step)]
        if step == 1:
            total = jnp.concatenate([total[:, : 2 * K], total[:, 2 * K :]], axis=0)
        if step < ITERS:
            gram = total[:, K * step : K + K * step]
        else:
            gram = jnp.concatenate([total[K:, i * K : (i + 1) * K] for i in range(4)], axis=0)
        products_before = total[0:K, : K * step]
        coef = dot_t(products_before, trans[0 : K * step, 0 : K * step], HIGHEST)
        return products_before, coef, gram - dot_t(coef, coef, HIGHEST)

    def settle(gram):
        gram_ref[...] = gram
        return gram_ref[...]

    def scaled(step, coef, gram):
        if step > 1:
            coef = dot(inverses[step - 1], coef, HIGHEST)
            gram = dot_t(dot(inverses[step - 1], gram, HIGHEST), inverses[step - 1], HIGHEST)
        return coef, settle(gram)

    def normalise(step, coef, gram):
        with phase("cholesky"):
            upper, inverse = cholesky(gram)
        if step > 0:
            fact_ref[step - 1] = upper.T
        if step < ITERS:
            own = inverse if step < 2 else dot(inverse, inverses[step - 1], HIGHEST)
            trans[K * step : K + K * step, K * step : K + K * step] = own
            if step > 0:
                trans[K * step : K + K * step, 0 : K * step] = -dot(
                    inverse,
                    dot(coef, trans[0 : K * step, 0 : K * step], HIGHEST),
                    HIGHEST,
                )
        uppers[step] = upper
        inverses[step] = inverse

    def record(step, coef):
        row = lax.broadcasted_iota(jnp.int32, (K, K), 0)
        col = lax.broadcasted_iota(jnp.int32, (K, K), 1)
        at = K * (step - 1)
        if step > 1:
            if step > 2:
                proj_ref[step - 1, :, 0 : at - K] = coef[:, : at - K]
            proj_ref[step - 1, :, at - K : at] = coef[:, at - K : at] + uppers[step - 1]
        proj_ref[step - 1, :, at : at + K] = coef[:, at:] + jnp.where(row == col, SHIFT, 0.0)

    uppers = {}
    inverses = {}
    scope = phase
    ahead = None
    for step in range(ITERS):
        size = height(step)
        if ahead is not None:
            newest = ahead()
        if step == 0:
            with scope("enter"):
                pl.semaphore_wait(barrier, len(FAR_FIRST) + len(SMALL_GROUP))
            mine = start_gram.at[core]
            remote(mine, mine, pair_gram_send, pair_gram_recv, g, partner).start()
            send_cols(0)
            with scope("load"):
                load.wait()
                table.wait()
            with scope("back"):
                products_of(lambda k: rows_0[rows_smem[0, 0, k]], size, tiles)
        else:
            with scope("wait_rows"):
                await_recv(rows_x[step].at[pl.ds(0, 3)], rows_send, rows_recv.at[step % 2])
            send_raw(step)
            with scope("back"):
                products_of(lambda k, step=step: rows_x[step][rows_smem[0, 0, k]], size, tiles)
        with scope("pairs"):
            send_pairs(step)
        with scope("own_sums"):
            own_sums(step)
            if step == 0:
                send_start_gram()
        if step == 0:
            with scope("turn"):

                def turn(k, carry):
                    turned[k] = tiles[k].T
                    return carry

                lax.fori_loop(0, TILES, turn, 0, unroll=2)

        @pl.when(core == 0)
        def _(step=step):
            send_back(step)

        with scope("wait_cols"):
            receive_cols(step)
        if step > 0:
            with scope("dots"):
                send_dots(step)

        @pl.when(core == 1)
        def _(step=step):
            send_back(step)

        with scope("wait_relay"):
            await_recv(cols_x[step].at[pl.ds(0, CHIPS)], relay_send, relay_recv.at[step % 2])
        with scope("forward"):
            products_of(lambda k, step=step: cols_x[step][cols_smem[0, 0, k]], size, turned)
        with scope("direct"):
            send_direct(step)

        if step == 0:
            with scope("wait_dots"):
                coef, gram = None, receive_start_gram()
            normalise(0, None, gram)
            first = dot(inverses[0], raw_x[g, 0:K, :], HIGHEST)
            known = first * (-SHIFT)
            basis[0:K, 0:BS] = first
        else:
            before, coef, gram = receive_dots(step)
            with scope("known"):
                known = raw_x[g, K * step : K * step + K, :] * (-SHIFT)
                known = known - dot(before, in_blocks[0 : K * step, :], HIGHEST)
                known = known - dot(gram, newest, HIGHEST)

        sent(step)
        with scope("wait_direct"):
            await_recv(
                direct_in.at[step, pl.ds(0, 3)], direct_send, direct_recv.at[step % 2]
            )
        with scope("wait_back"):
            await_recv(
                back_in.at[step, pl.ds(0, CHIPS - 1)], back_send, back_recv.at[step % 2]
            )
        with scope("update"):
            total = own_direct[...]
            for dy in (1, 2, 3):
                total = total + direct_in[step, lax.rem(g + dy, GRP)].astype(F32)
            total = total + own_back[chip] + pair_in[step, chip].astype(F32)
            for dz, dx in FAR_FIRST:
                total = total + back_in[step, chip_at(dz, dx)].astype(F32)
            image = 0.5 * total - raw_x[g, K * step : K * step + K, :] * dual
            if step == 0:
                image = dot(inverses[0], image, HIGHEST)
                basis[0:K, BS:] = image
                following = image + known
            elif step == 1:
                following = image + known
            else:
                following = dot(inverses[step - 1], image + known, HIGHEST)
            rounded = following.astype(BF16)
            after = step + 1
            raw_x[g, K * after : K * after + K, :] = following
            if after < ITERS:
                cols_x[after][r] = rounded
                rows_x[after][g] = rounded
                mine = rows_x[after].at[g]
                for dy in (2, 1, 3):
                    remote(
                        mine,
                        mine,
                        rows_send,
                        rows_recv.at[after % 2],
                        lax.rem(g + dy, GRP),
                        r,
                    ).start()
                send_cols(after)
            else:
                send_last()
                send_raw(after)

        def ahead(step=step, coef=coef, gram=gram, image=image):
            at = K * step
            if step > 0:
                coef, gram = scaled(step, coef, gram)
                normalise(step, coef, gram)
                both = jnp.concatenate([raw_x[g, at : at + K, :], image], axis=1)
                if step > 1:
                    both = dot(inverses[step - 1], both, HIGHEST)
                both = both - dot(coef, basis[0:at, :], HIGHEST)
                basis[at : at + K, :] = dot(inverses[step], both, HIGHEST)
                record(step, coef)
            if step == ITERS - 1:
                return None
            size = at + K
            in_blocks[0:size, :] = t_dot(
                trans[0:size, 0:size],
                basis[0:size, BS:] - SHIFT * basis[0:size, 0:BS],
                HIGHEST,
            )
            last = basis[at : at + K, 0:BS]
            return last if step == 0 else t_dot(inverses[step], last, HIGHEST)

    ahead()
    for i in range(GRP):
        old_rows[:, i * BS : (i + 1) * BS] = dot(trans[...], raw_x[i, 0 : K * ITERS, :], HIGHEST)
    receive_raw(ITERS)
    with scope("wait_last"):
        spread_last()
    _, coef, gram = receive_dots(ITERS)
    gram = settle(gram)
    for i in range(GRP):
        here = slice(i * BS, (i + 1) * BS)
        next_ref[:, here] = raw_x[i, K * ITERS :, :] - dot(coef, old_rows[:, here], HIGHEST)
    with scope("cholesky"):
        upper, inverse = cholesky(gram)
    with scope("final"):
        next_ref[...] = dot(inverse, next_ref[...], HIGHEST)
        fact_ref[ITERS - 1] = dot_t(inverses[ITERS - 1], upper, HIGHEST)
        record(ITERS, dot(inverses[ITERS - 1], coef, HIGHEST))

    await_send(last.at[pl.ds(0, CHIPS - 1)], last_send, last_recv)
    await_send(start_gram.at[0], pair_gram_send, pair_gram_recv)
    await_send(start_grams.at[pl.ds(0, CHIPS - 1)], gram_send, gram_recv)
    await_send(dots.at[ITERS, pl.ds(0, 7)], dots_send, dots_recv.at[0])


def write_out(*refs):
    inputs, outputs, sems = refs[:3], refs[3:6], refs[6]
    copies = [pltpu.make_async_copy(inputs[i], outputs[i], sems.at[i]) for i in (2, 0, 1)]
    for copy in copies:
        copy.start()
    for copy in copies:
        copy.wait()


def per_device(tiles, tile_rows, tile_cols, live_tiles, dual_shift, start_block):
    hbm = pl.BlockSpec(memory_space=pltpu.HBM)
    vmem = pl.BlockSpec(memory_space=pltpu.VMEM)
    in_hbm = functools.partial(pltpu.with_memory_space_constraint, memory_space=pltpu.HBM)
    dma = pltpu.SemaphoreType.DMA
    steps = ITERS + 1
    out = pl.pallas_call(
        kernel,
        out_shape=(
            pltpu.VMEM((ITERS, K, ITERS * K), F32),
            pltpu.VMEM((ITERS, K, K), F32),
            pltpu.VMEM((K, GRP * BS), F32),
        ),
        in_specs=[hbm] * 6,
        out_specs=(vmem, vmem, vmem),
        scratch_shapes=[
            pltpu.SMEM((1, 1, TILES), jnp.int32),
            pltpu.SMEM((1, 1, TILES), jnp.int32),
            pltpu.SMEM((1, 1), jnp.int32),
            pltpu.VMEM((1, GRP * BS), F32),
            pltpu.VMEM((K, K), F32),
            pltpu.VMEM((2, 8, 128), F32),
            pltpu.VMEM((CHIPS, 8, 128), F32),
            pltpu.VMEM((1, GRP * ROW), jnp.int32),
            pltpu.SMEM((1, GRP * ROW), jnp.int32),
            pltpu.VMEM((K, GRP * BS), F32),
            pltpu.VMEM((TILES, BS, BS), BF16),
            pltpu.VMEM((TILES, BS, BS), BF16),
            *[pltpu.VMEM((ROW, height(step), BS), BF16) for step in range(ITERS)],
            *[pltpu.VMEM((GRP, height(step), BS), BF16) for step in range(ITERS)],
            pltpu.VMEM((GRP, K * steps, BS), F32),
            pltpu.VMEM((K * ITERS, 2 * BS), F32),
            pltpu.VMEM((K * ITERS, BS), F32),
            pltpu.VMEM((K * ITERS, GRP * BS), F32),
            pltpu.VMEM((K * ITERS, K * ITERS), F32),
            pltpu.VMEM((TILES + 1, K, BS), F32),
            pltpu.VMEM((ITERS, CHIPS, K, BS), BF16),
            pltpu.VMEM((ITERS, CHIPS, K, BS), BF16),
            pltpu.VMEM((ITERS, CHIPS, K, BS), BF16),
            pltpu.VMEM((ITERS, CHIPS, K, BS), BF16),
            pltpu.VMEM((CHIPS, K, BS), F32),
            pltpu.VMEM((K, BS), F32),
            pltpu.VMEM((ITERS, GRP, K, BS), BF16),
            pltpu.VMEM((ITERS, GRP, K, BS), BF16),
            pltpu.VMEM((steps, 2 * GRP, K + 8, 128), F32),
            pltpu.VMEM((CHIPS, K + 8, 128), F32),
            dma((5,)),
            dma,
            dma,
            dma,
            dma,
            dma,
            dma,
            dma,
            dma,
            dma,
            dma((2, len(WAVES))),
            *[dma, dma((2,))] * 7,
        ],
        compiler_params=pltpu.CompilerParams(
            collective_id=0, has_side_effects=True, vmem_limit_bytes=48 * 1024 * 1024
        ),
        name="lanczos",
    )(
        in_hbm(tile_rows),
        in_hbm(tile_cols),
        live_tiles,
        *[
            in_hbm(a)
            for a in (
                tiles.reshape(TILES, BS, BS),
                start_block,
                dual_shift.reshape(1, GRP * BS),
            )
        ]
    )
    return pl.pallas_call(
        write_out,
        out_shape=tuple(jax.ShapeDtypeStruct(a.shape, a.dtype) for a in out),
        in_specs=[vmem] * 3,
        out_specs=(hbm, hbm, hbm),
        scratch_shapes=[dma((3,))],
        compiler_params=pltpu.CompilerParams(vmem_limit_bytes=1024 * 1024),
        name="write_out",
    )(*[pltpu.with_memory_space_constraint(a, pltpu.VMEM) for a in out])


def solution(mesh):
    in_specs = (
        P("grp", "row", None, None, None),
        P("grp", "row", None),
        P("grp", "row", None),
        P("grp", "row"),
        P("row"),
        P(None, "row"),
    )
    out_specs = (P(), P(), P(None, "row"))
    return jax.shard_map(
        per_device, mesh=mesh, in_specs=in_specs, out_specs=out_specs, check_vma=False
    )
```
